128 devices in a mesh: gossip: 32 (over z, y_lo, x), mp: 4 (over y_hi, core).
Axes of the slice: x: 4, y: 4 (y_hi: 2, y_lo: 2; y = y_hi * 2 + y_lo), z: 4, core: 2. Of those that a mesh axis runs over, the one named last changes fastest.
Arguments:
- tokens: bfloat16 [32, 512, 2048], P('gossip'), may hold values from -6 to 6
- targets: bfloat16 [32, 512, 2048], P('gossip'), may hold values from -6 to 6
- gate_weight: bfloat16 [32, 2048, 4096], P('gossip', None, 'mp'), may hold values from -6 to 6
- up_weight: bfloat16 [32, 2048, 4096], P('gossip', None, 'mp'), may hold values from -6 to 6
- down_weight: bfloat16 [32, 4096, 2048], P('gossip', 'mp'), may hold values from -6 to 6
Outputs:
- gate_out: bfloat16 [32, 2048, 4096], P('gossip', None, 'mp')
- up_out: bfloat16 [32, 2048, 4096], P('gossip', None, 'mp')
- down_out: bfloat16 [32, 4096, 2048], P('gossip', 'mp')
The draws below stay inside these ranges and needn't reach their ends.
All inputs are finite; a program needn't handle non-finite values.
Results may differ from the reference program's by a relative error of at most 0.0095.
Values may be sent and summed in bfloat16 or wider, within the bound.
A program may use at most 128 MiB of HBM per device.

```python
import jax
import jax.numpy as jnp
from jax import lax

D = 2048
TOK = 512
ITERS = 1
FF = 4096
REPLICAS = 32


def levels(own_key, dims, pieces, least, largest):
    gain = 1.0
    for dim, blocks in pieces:
        steps = jax.random.uniform(jax.random.fold_in(jax.random.fold_in(own_key, 6), dim), (blocks,), jnp.float32, least / len(pieces), largest / len(pieces))
        gain = gain * jnp.repeat(jnp.exp(steps), dims[dim] // blocks).reshape((-1,) + (1,) * (len(dims) - 1 - dim))
    return gain


def bell_draw(stream_key, extent, spread, reach, split=(), kind=jnp.bfloat16):
    values = spread * jax.random.normal(stream_key, extent, jnp.float32)
    if split:
        values = values * levels(stream_key, extent, split, -0.22, 0.18)
    return jnp.clip(values, -reach, reach).astype(kind)


def setup_inputs(seed: int = 0) -> dict:
    keys = jax.random.split(jax.random.key(seed), 6)
    return {
        "tokens": bell_draw(keys[0], (REPLICAS, TOK, D), 1.0, 6.0, ((0, 32),)),
        "targets": bell_draw(keys[1], (REPLICAS, TOK, D), 1.0, 6.0, ((0, 32),)),
        "gate_weight": bell_draw(keys[2], (REPLICAS, D, FF), 1.0, 6.0, ((0, 32), (2, 4))),
        "up_weight": bell_draw(keys[3], (REPLICAS, D, FF), 1.0, 6.0, ((0, 32), (2, 4))),
        "down_weight": bell_draw(keys[4], (REPLICAS, FF, D), 1.0, 6.0, ((0, 32), (1, 4))),
    }


def rms_norm(values):
    widened = values.astype(jnp.float32)
    return (widened * lax.rsqrt(lax.optimization_barrier(jnp.mean(widened * widened, axis=-1, keepdims=True)) + 1e-06)).astype(jnp.bfloat16)

def mix_cycle(stepped):
    widened = stepped.astype(jnp.float32)
    total = jnp.roll(widened, 1, axis=0) + widened + jnp.roll(widened, -1, axis=0)
    return (total / 3.0).astype(jnp.bfloat16)

def reference(tokens, targets, gate_weight, up_weight, down_weight):
    tok_count = tokens.shape[1]
    width = tokens.shape[2]
    hidden_all = gate_weight.shape[2]
    in_scale = 1.0 / width ** 0.5
    mid_scale = 1.0 / hidden_all ** 0.5
    step_size = hidden_all / 4.0
    normed = rms_norm(tokens).astype(jnp.float32)
    offset = tokens.astype(jnp.float32) - targets.astype(jnp.float32)
    w_gate, w_up, w_down = (gate_weight, up_weight, down_weight)
    for iteration in range(ITERS):
        gate_pre = jnp.einsum('rtd,rdf->rtf', normed, w_gate.astype(jnp.float32)) * in_scale
        up_pre = jnp.einsum('rtd,rdf->rtf', normed, w_up.astype(jnp.float32)) * in_scale
        sig_gate = jax.nn.sigmoid(gate_pre)
        act_gate = gate_pre * sig_gate
        hidden = (act_gate * up_pre).astype(jnp.bfloat16).astype(jnp.float32)
        output = jnp.einsum('rtf,rfd->rtd', hidden, w_down.astype(jnp.float32)) * mid_scale
        err_grad = ((offset + output) / tok_count).astype(jnp.bfloat16).astype(jnp.float32)
        grad_down = jnp.einsum('rtf,rtd->rfd', hidden, err_grad) * mid_scale
        grad_hidden = jnp.einsum('rtd,rfd->rtf', err_grad, w_down.astype(jnp.float32)) * mid_scale
        grad_gate = (grad_hidden * up_pre * (sig_gate * (1.0 + gate_pre * (1.0 - sig_gate)))).astype(jnp.bfloat16).astype(jnp.float32)
        grad_up = (grad_hidden * act_gate).astype(jnp.bfloat16).astype(jnp.float32)
        grad_wgate = jnp.einsum('rtd,rtf->rdf', normed, grad_gate) * in_scale
        grad_wup = jnp.einsum('rtd,rtf->rdf', normed, grad_up) * in_scale
        new_gate = (w_gate.astype(jnp.float32) - step_size * grad_wgate).astype(jnp.bfloat16)
        new_up = (w_up.astype(jnp.float32) - step_size * grad_wup).astype(jnp.bfloat16)
        new_down = (w_down.astype(jnp.float32) - step_size * grad_down).astype(jnp.bfloat16)
        w_gate = mix_cycle(new_gate)
        w_up = mix_cycle(new_up)
        w_down = mix_cycle(new_down)
    return (w_gate, w_up, w_down)
```

```python
import functools

import jax
import jax.numpy as jnp
from jax import lax
from jax.experimental import pallas as pl
from jax.experimental.pallas import tpu as pltpu
from jax.sharding import PartitionSpec as P

MESH = pl.DeviceIdType.MESH
F32 = jnp.float32
BF16 = jnp.bfloat16
COLS = 256
ROWS = 256


def dot(a, b, dims):
    return lax.dot_general(a, b, (dims, ((), ())), preferred_element_type=F32)


def kernel(
    replicas,
    tok_h, tgt_h, wg_h, wu_h, wd_h,
    og, ou, od, lo_h, hi_h,
    x, tg, nrm, wd, slope, act, hid, hid_t, err, gg, gu,
    part, part_in, sum_in, glo, ghi, ulo, uhi, stage,
    load_sem, w_sem, p_send, p_recv, q_send, q_recv, e_send, e_recv,
    d_send, d_recv, g_send, g_recv, u_send, u_recv, st_sem,
):
    g = lax.axis_index("gossip")
    m = lax.axis_index("mp")
    core = lax.rem(m, 2)
    sibling = m + 1 - 2 * core
    peer = lax.rem(m + 2, 4)
    after = lax.rem(g + 1, replicas)
    before = lax.rem(g + replicas - 1, replicas)
    toks, width = x.shape
    units = wd.shape[0]
    half = toks // 2
    in_scale = 1.0 / width**0.5
    mid_scale = 1.0 / (4 * units) ** 0.5
    step_size = (4 * units) / 4.0
    n_cols = width // COLS
    n_rows = width // ROWS
    n_units = units // COLS
    mine = pl.ds(pl.multiple_of(core * half, half), half)
    theirs = pl.ds(pl.multiple_of((1 - core) * half, half), half)

    def cols(i, size=COLS):
        return pl.ds(pl.multiple_of(i * size, size), size)

    tok_copy = pltpu.make_async_copy(tok_h, x, load_sem.at[0])
    tok_copy.start()

    def w_copies(f):
        return (
            pltpu.make_async_copy(wg_h.at[:, cols(f)], og.at[:, cols(f)], w_sem.at[0, f]),
            pltpu.make_async_copy(wu_h.at[:, cols(f)], ou.at[:, cols(f)], w_sem.at[1, f]),
        )

    for f in range(n_units):
        for copy in w_copies(f):
            copy.start()
    wd_copy = pltpu.make_async_copy(wd_h, wd, load_sem.at[1])
    wd_copy.start()
    tgt_copy = pltpu.make_async_copy(tgt_h.at[mine, :], tg, load_sem.at[2])
    tgt_copy.start()

    barrier = pltpu.get_barrier_semaphore()
    for where in ((g, sibling), (g, peer), (after, m), (before, m)):
        pl.semaphore_signal(barrier, inc=1, device_id=where, device_id_type=MESH)

    tok_copy.wait()

    def norm(i, carry):
        rows = pl.ds(pl.multiple_of(i * 64, 64), 64)
        wide = x[rows, :].astype(F32)
        mean = jnp.mean(wide * wide, axis=-1, keepdims=True)
        nrm[rows, :] = (wide * lax.rsqrt(mean + 1e-06)).astype(BF16)
        return carry

    lax.fori_loop(0, toks // 64, norm, 0)

    def forward(f, carry):
        for copy in w_copies(f):
            copy.wait()
        gate = dot(nrm[...], og[:, cols(f)], ((1,), (0,))) * in_scale
        up = dot(nrm[...], ou[:, cols(f)], ((1,), (0,))) * in_scale
        sig = jax.nn.sigmoid(gate)
        acted = gate * sig
        act[:, cols(f)] = acted
        slope[:, cols(f)] = up * (sig * (1.0 + gate * (1.0 - sig)))
        hid[:, cols(f)] = (acted * up).astype(BF16)
        return carry

    lax.fori_loop(0, n_units, forward, 0)
    wd_copy.wait()
    pl.semaphore_wait(barrier, 4)

    def p_copy(d):
        return pltpu.make_async_remote_copy(
            src_ref=part.at[theirs, cols(d)], dst_ref=part_in.at[:, cols(d)],
            send_sem=p_send.at[d], recv_sem=p_recv.at[d],
            device_id=(g, sibling), device_id_type=MESH,
        )

    def q_copy(d):
        return pltpu.make_async_remote_copy(
            src_ref=part.at[mine, cols(d)], dst_ref=sum_in.at[:, cols(d)],
            send_sem=q_send.at[d], recv_sem=q_recv.at[d],
            device_id=(g, peer), device_id_type=MESH,
        )

    def e_copy(d):
        return pltpu.make_async_remote_copy(
            src_ref=err.at[mine, cols(d)], dst_ref=err.at[mine, cols(d)],
            send_sem=e_send.at[d], recv_sem=e_recv.at[d],
            device_id=(g, sibling), device_id_type=MESH,
        )

    def pair(src, lo, hi, send, recv, i):
        return (
            pltpu.make_async_remote_copy(
                src_ref=src, dst_ref=lo, send_sem=send.at[0, i], recv_sem=recv.at[0, i],
                device_id=(after, m), device_id_type=MESH,
            ),
            pltpu.make_async_remote_copy(
                src_ref=src, dst_ref=hi, send_sem=send.at[1, i], recv_sem=recv.at[1, i],
                device_id=(before, m), device_id_type=MESH,
            ),
        )

    def d_copies(d):
        return pair(od.at[:, cols(d)], lo_h.at[d], hi_h.at[d], d_send, d_recv, d)

    def g_copies(i):
        rows = cols(i, ROWS)
        return pair(og.at[rows, :], glo.at[rows, :], ghi.at[rows, :], g_send, g_recv, i)

    def u_copies(i):
        rows = cols(i, ROWS)
        return pair(ou.at[rows, :], ulo.at[rows, :], uhi.at[rows, :], u_send, u_recv, i)

    def partial(d):
        part[:, cols(d)] = dot(hid[...], wd[:, cols(d)], ((1,), (0,))).astype(BF16)
        p_copy(d).start()

    def join(d):
        p_copy(d).wait()
        total = part[mine, cols(d)].astype(F32) + part_in[:, cols(d)].astype(F32)
        part[mine, cols(d)] = total.astype(BF16)
        q_copy(d).start()

    partial(0)
    partial(1)

    def spread(i, carry):
        join(i)
        partial(i + 2)
        return carry

    lax.fori_loop(0, n_cols - 2, spread, 0)
    join(n_cols - 2)
    join(n_cols - 1)

    def turn(i, carry):
        hid_t[cols(i), :] = hid[:, cols(i)].T
        return carry

    lax.fori_loop(0, n_units, turn, 0)
    tgt_copy.wait()

    def down(d, carry):
        q_copy(d).wait()
        total = part[mine, cols(d)].astype(F32) + sum_in[:, cols(d)].astype(F32)
        offset = x[mine, cols(d)].astype(F32) - tg[:, cols(d)].astype(F32)
        err[mine, cols(d)] = ((offset + total * mid_scale) / toks).astype(BF16)
        e_copy(d).start()
        e_copy(d).wait()
        grad = dot(hid_t[...], err[:, cols(d)], ((1,), (0,)))
        od[:, cols(d)] = (
            wd[:, cols(d)].astype(F32) - (step_size * mid_scale) * grad
        ).astype(BF16)
        for copy in d_copies(d):
            copy.start()
        return carry

    lax.fori_loop(0, n_cols, down, 0)

    def back(f, carry):
        grad = dot(err[...], wd[cols(f), :], ((1,), (1,))) * mid_scale
        gg[:, cols(f)] = (grad * slope[:, cols(f)]).astype(BF16)
        gu[:, cols(f)] = (grad * act[:, cols(f)]).astype(BF16)
        return carry

    lax.fori_loop(0, n_units, back, 0)

    def step(out, grads, copies):
        def one(i, carry):
            rows = cols(i, ROWS)
            grad = dot(nrm[:, rows], grads[...], ((0,), (0,)))
            out[rows, :] = (
                out[rows, :].astype(F32) - (step_size * in_scale) * grad
            ).astype(BF16)
            for copy in copies(i):
                copy.start()
            return carry

        lax.fori_loop(0, n_rows, one, 0)

    step(og, gg, g_copies)
    step(ou, gu, u_copies)

    def third(lo, own, hi):
        return ((lo.astype(F32) + own.astype(F32) + hi.astype(F32)) / 3.0).astype(BF16)

    def mix_down(d, carry):
        for copy in d_copies(d):
            copy.wait()
        loads = [
            pltpu.make_async_copy(lo_h.at[d], stage.at[0], st_sem.at[0]),
            pltpu.make_async_copy(hi_h.at[d], stage.at[1], st_sem.at[1]),
        ]
        for load in loads:
            load.start()
        for load in loads:
            load.wait()
        od[:, cols(d)] = third(stage[0], od[:, cols(d)], stage[1])
        return carry

    lax.fori_loop(0, n_cols, mix_down, 0)

    def mix(out, lo, hi, copies):
        def one(i, carry):
            rows = cols(i, ROWS)
            for copy in copies(i):
                copy.wait()
            out[rows, :] = third(lo[rows, :], out[rows, :], hi[rows, :])
            return carry

        lax.fori_loop(0, n_rows, one, 0)

    mix(og, glo, ghi, g_copies)
    mix(ou, ulo, uhi, u_copies)


def local(replicas, tokens, targets, gate_weight, up_weight, down_weight):
    toks, width = tokens.shape[1:]
    units = gate_weight.shape[2]
    n_cols, n_rows, n_units = width // COLS, width // ROWS, units // COLS
    half = toks // 2
    dma = pltpu.SemaphoreType.DMA
    any_spec = pl.BlockSpec(memory_space=pl.ANY)
    vmem_spec = pl.BlockSpec(memory_space=pltpu.VMEM)
    received = jax.ShapeDtypeStruct((n_cols, units, COLS), BF16)
    gate_out, up_out, down_out, _, _ = pl.pallas_call(
        functools.partial(kernel, replicas),
        out_shape=(
            pltpu.VMEM((width, units), BF16),
            pltpu.VMEM((width, units), BF16),
            pltpu.VMEM((units, width), BF16),
            received,
            received,
        ),
        in_specs=[any_spec] * 5,
        out_specs=(vmem_spec, vmem_spec, vmem_spec, any_spec, any_spec),
        scratch_shapes=[
            pltpu.VMEM((toks, width), BF16),
            pltpu.VMEM((half, width), BF16),
            pltpu.VMEM((toks, width), BF16),
            pltpu.VMEM((units, width), BF16),
            pltpu.VMEM((toks, units), F32),
            pltpu.VMEM((toks, units), F32),
            pltpu.VMEM((toks, units), BF16),
            pltpu.VMEM((units, toks), BF16),
            pltpu.VMEM((toks, width), BF16),
            pltpu.VMEM((toks, units), BF16),
            pltpu.VMEM((toks, units), BF16),
            pltpu.VMEM((toks, width), BF16),
            pltpu.VMEM((half, width), BF16),
            pltpu.VMEM((half, width), BF16),
            pltpu.VMEM((width, units), BF16),
            pltpu.VMEM((width, units), BF16),
            pltpu.VMEM((width, units), BF16),
            pltpu.VMEM((width, units), BF16),
            pltpu.VMEM((2, units, COLS), BF16),
            dma((3,)),
            dma((2, n_units)),
            dma((n_cols,)),
            dma((n_cols,)),
            dma((n_cols,)),
            dma((n_cols,)),
            dma((n_cols,)),
            dma((n_cols,)),
            dma((2, n_cols)),
            dma((2, n_cols)),
            dma((2, n_rows)),
            dma((2, n_rows)),
            dma((2, n_rows)),
            dma((2, n_rows)),
            dma((2,)),
        ],
        compiler_params=pltpu.CompilerParams(
            collective_id=0, has_side_effects=True, vmem_limit_bytes=50 * 2**20
        ),
    )(tokens[0], targets[0], gate_weight[0], up_weight[0], down_weight[0])
    return gate_out[None], up_out[None], down_out[None]


def solution(mesh):
    placed = (
        P("gossip", None, None),
        P("gossip", None, None),
        P("gossip", None, "mp"),
        P("gossip", None, "mp"),
        P("gossip", "mp", None),
    )
    return jax.shard_map(
        functools.partial(local, mesh.shape["gossip"]),
        mesh=mesh,
        in_specs=placed,
        out_specs=(P("gossip", None, "mp"), P("gossip", None, "mp"), P("gossip", "mp", None)),
        check_vma=False,
    )
```

```python
import functools

import jax
import jax.numpy as jnp
from jax import lax
from jax.experimental import pallas as pl
from jax.experimental.pallas import tpu as pltpu
from jax.sharding import PartitionSpec as P

MESH = pl.DeviceIdType.MESH
F32 = jnp.float32
BF16 = jnp.bfloat16
COLS = 256
X, Y = 4, 2
ROWS = 256


def dot(a, b, dims):
    return lax.dot_general(a, b, (dims, ((), ())), preferred_element_type=F32)


def kernel(
    replicas,
    tok_h, tgt_h, wg_h, wu_h, wd_h,
    og, ou, od, lo_h, hi_h,
    x, tg, nrm, wd, slope, act, hid, hid_t, err, gg, gu,
    part, part_in, sum_in, glo, ghi, ulo, uhi, stage,
    load_sem, w_sem, p_send, p_recv, q_send, q_recv, e_send, e_recv,
    d_send, d_recv, g_send, g_recv, u_send, u_recv, st_sem, go_sem,
):
    g = lax.axis_index("gossip")
    m = lax.axis_index("mp")
    core = lax.rem(m, 2)
    sibling = m + 1 - 2 * core
    peer = lax.rem(m + 2, 4)
    after = lax.rem(g + 1, replicas)
    before = lax.rem(g + replicas - 1, replicas)
    toks, width = x.shape
    units = wd.shape[0]
    half = toks // 2
    in_scale = 1.0 / width**0.5
    mid_scale = 1.0 / (4 * units) ** 0.5
    step_size = (4 * units) / 4.0
    n_cols = width // COLS
    n_rows = width // ROWS
    n_units = units // COLS
    mine = pl.ds(pl.multiple_of(core * half, half), half)
    theirs = pl.ds(pl.multiple_of((1 - core) * half, half), half)

    def cols(i, size=COLS):
        return pl.ds(pl.multiple_of(i * size, size), size)

    tok_copy = pltpu.make_async_copy(tok_h, x, load_sem.at[0])
    tok_copy.start()

    def w_copies(f):
        return (
            pltpu.make_async_copy(wg_h.at[:, cols(f)], og.at[:, cols(f)], w_sem.at[0, f]),
            pltpu.make_async_copy(wu_h.at[:, cols(f)], ou.at[:, cols(f)], w_sem.at[1, f]),
        )

    for f in range(n_units):
        for copy in w_copies(f):
            copy.start()
    wd_copy = pltpu.make_async_copy(wd_h, wd, load_sem.at[1])
    wd_copy.start()
    tgt_copy = pltpu.make_async_copy(tgt_h.at[mine, :], tg, load_sem.at[2])
    tgt_copy.start()

    along = lax.rem(g, X)
    last_end = along == X - 1
    first_end = along == 0
    at_end = jnp.logical_or(last_end, first_end)
    layer = g // (X * Y)
    layers = replicas // (X * Y)
    beyond = lax.rem(layer + (along // (X - 1)) * 2 - 1 + layers, layers)
    facing = [
        (at * (X * Y) + row * X + (X - 1 - along), shard)
        for at in (layer, beyond)
        for row in range(Y)
        for shard in range(4)
    ]

    def tell(sem, wheres):
        for where in wheres:
            pl.semaphore_signal(sem, inc=1, device_id=where, device_id_type=MESH)

    barrier = pltpu.get_barrier_semaphore()
    near = ((g, sibling), (g, peer))
    inward = g + 1 - 2 * (along // (X - 1))

    @pl.when(jnp.logical_not(at_end))
    def _():
        tell(barrier, (*near, (after, m), (before, m)))

    @pl.when(at_end)
    def _():
        tell(barrier, (*near, (inward, m), *facing))

    tok_copy.wait()

    def norm(i, carry):
        rows = pl.ds(pl.multiple_of(i * 64, 64), 64)
        wide = x[rows, :].astype(F32)
        mean = jnp.mean(wide * wide, axis=-1, keepdims=True)
        nrm[rows, :] = (wide * lax.rsqrt(mean + 1e-06)).astype(BF16)
        return carry

    lax.fori_loop(0, toks // 64, norm, 0)

    def forward(f, carry):
        for copy in w_copies(f):
            copy.wait()
        gate = dot(nrm[...], og[:, cols(f)], ((1,), (0,))) * in_scale
        up = dot(nrm[...], ou[:, cols(f)], ((1,), (0,))) * in_scale
        sig = jax.nn.sigmoid(gate)
        acted = gate * sig
        act[:, cols(f)] = acted
        slope[:, cols(f)] = up * (sig * (1.0 + gate * (1.0 - sig)))
        hid[:, cols(f)] = (acted * up).astype(BF16)
        return carry

    lax.fori_loop(0, n_units, forward, 0)
    wd_copy.wait()

    @pl.when(jnp.logical_not(at_end))
    def _():
        pl.semaphore_wait(barrier, len(near) + 2)

    @pl.when(at_end)
    def _():
        pl.semaphore_wait(barrier, len(near) + 1 + len(facing))

    def p_copy(d):
        return pltpu.make_async_remote_copy(
            src_ref=part.at[theirs, cols(d)], dst_ref=part_in.at[:, cols(d)],
            send_sem=p_send.at[d], recv_sem=p_recv.at[d],
            device_id=(g, sibling), device_id_type=MESH,
        )

    def q_copy(d):
        return pltpu.make_async_remote_copy(
            src_ref=part.at[mine, cols(d)], dst_ref=sum_in.at[:, cols(d)],
            send_sem=q_send.at[d], recv_sem=q_recv.at[d],
            device_id=(g, peer), device_id_type=MESH,
        )

    def e_copy(d):
        return pltpu.make_async_remote_copy(
            src_ref=err.at[mine, cols(d)], dst_ref=err.at[mine, cols(d)],
            send_sem=e_send.at[d], recv_sem=e_recv.at[d],
            device_id=(g, sibling), device_id_type=MESH,
        )

    def pair(src, lo, hi, send, recv, i):
        return (
            pltpu.make_async_remote_copy(
                src_ref=src, dst_ref=lo, send_sem=send.at[0, i], recv_sem=recv.at[0, i],
                device_id=(after, m), device_id_type=MESH,
            ),
            pltpu.make_async_remote_copy(
                src_ref=src, dst_ref=hi, send_sem=send.at[1, i], recv_sem=recv.at[1, i],
                device_id=(before, m), device_id_type=MESH,
            ),
        )

    def d_copies(d):
        return pair(od.at[:, cols(d)], lo_h.at[d], hi_h.at[d], d_send, d_recv, d)

    def g_copies(i):
        rows = cols(i, ROWS)
        return pair(og.at[rows, :], glo.at[rows, :], ghi.at[rows, :], g_send, g_recv, i)

    def u_copies(i):
        rows = cols(i, ROWS)
        return pair(ou.at[rows, :], ulo.at[rows, :], uhi.at[rows, :], u_send, u_recv, i)

    def partial(d):
        part[:, cols(d)] = dot(hid[...], wd[:, cols(d)], ((1,), (0,))).astype(BF16)
        p_copy(d).start()

    def join(d):
        p_copy(d).wait()
        total = part[mine, cols(d)].astype(F32) + part_in[:, cols(d)].astype(F32)
        part[mine, cols(d)] = total.astype(BF16)
        q_copy(d).start()

    partial(0)
    partial(1)

    def spread(i, carry):
        join(i)
        partial(i + 2)
        return carry

    lax.fori_loop(0, n_cols - 2, spread, 0)
    join(n_cols - 2)
    join(n_cols - 1)

    def turn(i, carry):
        hid_t[cols(i), :] = hid[:, cols(i)].T
        return carry

    lax.fori_loop(0, n_units, turn, 0)
    tgt_copy.wait()

    def down(d, carry):
        q_copy(d).wait()

        @pl.when(jnp.logical_and(at_end, d == n_cols - 1))
        def _():
            tell(go_sem, facing)

        total = part[mine, cols(d)].astype(F32) + sum_in[:, cols(d)].astype(F32)
        offset = x[mine, cols(d)].astype(F32) - tg[:, cols(d)].astype(F32)
        err[mine, cols(d)] = ((offset + total * mid_scale) / toks).astype(BF16)
        e_copy(d).start()
        e_copy(d).wait()
        grad = dot(hid_t[...], err[:, cols(d)], ((1,), (0,)))
        od[:, cols(d)] = (
            wd[:, cols(d)].astype(F32) - (step_size * mid_scale) * grad
        ).astype(BF16)
        ahead, behind = d_copies(d)
        pl.when(jnp.logical_not(last_end))(ahead.start)
        pl.when(jnp.logical_not(first_end))(behind.start)
        return carry

    lax.fori_loop(0, n_cols, down, 0)

    @pl.when(at_end)
    def _():
        pl.semaphore_wait(go_sem, len(facing))

    def held_back(d, carry):
        ahead, behind = d_copies(d)
        pl.when(last_end)(ahead.start)
        pl.when(first_end)(behind.start)
        return carry

    lax.fori_loop(0, n_cols, held_back, 0)

    def back(f, carry):
        grad = dot(err[...], wd[cols(f), :], ((1,), (1,))) * mid_scale
        gg[:, cols(f)] = (grad * slope[:, cols(f)]).astype(BF16)
        gu[:, cols(f)] = (grad * act[:, cols(f)]).astype(BF16)
        return carry

    lax.fori_loop(0, n_units, back, 0)

    def step(out, grads, copies):
        def one(i, carry):
            rows = cols(i, ROWS)
            grad = dot(nrm[:, rows], grads[...], ((0,), (0,)))
            out[rows, :] = (
                out[rows, :].astype(F32) - (step_size * in_scale) * grad
            ).astype(BF16)
            for copy in copies(i):
                copy.start()
            return carry

        lax.fori_loop(0, n_rows, one, 0)

    step(og, gg, g_copies)
    step(ou, gu, u_copies)

    def third(lo, own, hi):
        return ((lo.astype(F32) + own.astype(F32) + hi.astype(F32)) / 3.0).astype(BF16)

    def mix_down(d, carry):
        for copy in d_copies(d):
            copy.wait()
        loads = [
            pltpu.make_async_copy(lo_h.at[d], stage.at[0], st_sem.at[0]),
            pltpu.make_async_copy(hi_h.at[d], stage.at[1], st_sem.at[1]),
        ]
        for load in loads:
            load.start()
        for load in loads:
            load.wait()
        od[:, cols(d)] = third(stage[0], od[:, cols(d)], stage[1])
        return carry

    lax.fori_loop(0, n_cols, mix_down, 0)

    def mix(out, lo, hi, copies):
        def one(i, carry):
            rows = cols(i, ROWS)
            for copy in copies(i):
                copy.wait()
            out[rows, :] = third(lo[rows, :], out[rows, :], hi[rows, :])
            return carry

        lax.fori_loop(0, n_rows, one, 0)

    mix(og, glo, ghi, g_copies)
    mix(ou, ulo, uhi, u_copies)


def local(replicas, tokens, targets, gate_weight, up_weight, down_weight):
    toks, width = tokens.shape[1:]
    units = gate_weight.shape[2]
    n_cols, n_rows, n_units = width // COLS, width // ROWS, units // COLS
    half = toks // 2
    dma = pltpu.SemaphoreType.DMA
    any_spec = pl.BlockSpec(memory_space=pl.ANY)
    vmem_spec = pl.BlockSpec(memory_space=pltpu.VMEM)
    received = jax.ShapeDtypeStruct((n_cols, units, COLS), BF16)
    gate_out, up_out, down_out, _, _ = pl.pallas_call(
        functools.partial(kernel, replicas),
        out_shape=(
            pltpu.VMEM((width, units), BF16),
            pltpu.VMEM((width, units), BF16),
            pltpu.VMEM((units, width), BF16),
            received,
            received,
        ),
        in_specs=[any_spec] * 5,
        out_specs=(vmem_spec, vmem_spec, vmem_spec, any_spec, any_spec),
        scratch_shapes=[
            pltpu.VMEM((toks, width), BF16),
            pltpu.VMEM((half, width), BF16),
            pltpu.VMEM((toks, width), BF16),
            pltpu.VMEM((units, width), BF16),
            pltpu.VMEM((toks, units), F32),
            pltpu.VMEM((toks, units), F32),
            pltpu.VMEM((toks, units), BF16),
            pltpu.VMEM((units, toks), BF16),
            pltpu.VMEM((toks, width), BF16),
            pltpu.VMEM((toks, units), BF16),
            pltpu.VMEM((toks, units), BF16),
            pltpu.VMEM((toks, width), BF16),
            pltpu.VMEM((half, width), BF16),
            pltpu.VMEM((half, width), BF16),
            pltpu.VMEM((width, units), BF16),
            pltpu.VMEM((width, units), BF16),
            pltpu.VMEM((width, units), BF16),
            pltpu.VMEM((width, units), BF16),
            pltpu.VMEM((2, units, COLS), BF16),
            dma((3,)),
            dma((2, n_units)),
            dma((n_cols,)),
            dma((n_cols,)),
            dma((n_cols,)),
            dma((n_cols,)),
            dma((n_cols,)),
            dma((n_cols,)),
            dma((2, n_cols)),
            dma((2, n_cols)),
            dma((2, n_rows)),
            dma((2, n_rows)),
            dma((2, n_rows)),
            dma((2, n_rows)),
            dma((2,)),
            pltpu.SemaphoreType.REGULAR,
        ],
        compiler_params=pltpu.CompilerParams(
            collective_id=0, has_side_effects=True, vmem_limit_bytes=50 * 2**20
        ),
    )(tokens[0], targets[0], gate_weight[0], up_weight[0], down_weight[0])
    return gate_out[None], up_out[None], down_out[None]


def solution(mesh):
    placed = (
        P("gossip", None, None),
        P("gossip", None, None),
        P("gossip", None, "mp"),
        P("gossip", None, "mp"),
        P("gossip", "mp", None),
    )
    return jax.shard_map(
        functools.partial(local, mesh.shape["gossip"]),
        mesh=mesh,
        in_specs=placed,
        out_specs=(P("gossip", None, "mp"), P("gossip", None, "mp"), P("gossip", "mp", None)),
        check_vma=False,
    )
```

```python
import functools

import jax
import jax.numpy as jnp
from jax import lax
from jax.experimental import pallas as pl
from jax.experimental.pallas import tpu as pltpu
from jax.sharding import PartitionSpec as P

MESH = pl.DeviceIdType.MESH
F32 = jnp.float32
BF16 = jnp.bfloat16
COLS = 256
X, Y = 4, 2
ROWS = 256


def dot(a, b, dims):
    return lax.dot_general(a, b, (dims, ((), ())), preferred_element_type=F32)


def kernel(
    replicas,
    tok_h, tgt_h, wg_h, wu_h, wd_h,
    og, ou, od, lo_h, hi_h, relay_h,
    x, tg, nrm, wd, slope, act, hid, hid_t, err, gg, gu,
    part, part_in, sum_in, glo, ghi, ulo, uhi, stage,
    load_sem, w_sem, p_send, p_recv, q_send, q_recv, e_send, e_recv,
    d_send, d_recv, g_send, g_recv, u_send, u_recv, st_sem, relay_sem, go_sem,
):
    g = lax.axis_index("gossip")
    m = lax.axis_index("mp")
    core = lax.rem(m, 2)
    sibling = m + 1 - 2 * core
    peer = lax.rem(m + 2, 4)
    after = lax.rem(g + 1, replicas)
    before = lax.rem(g + replicas - 1, replicas)
    toks, width = x.shape
    units = wd.shape[0]
    half = toks // 2
    in_scale = 1.0 / width**0.5
    mid_scale = 1.0 / (4 * units) ** 0.5
    step_size = (4 * units) / 4.0
    n_cols = width // COLS
    n_rows = width // ROWS
    n_units = units // COLS
    mine = pl.ds(pl.multiple_of(core * half, half), half)
    theirs = pl.ds(pl.multiple_of((1 - core) * half, half), half)

    def cols(i, size=COLS):
        return pl.ds(pl.multiple_of(i * size, size), size)

    tok_copy = pltpu.make_async_copy(tok_h, x, load_sem.at[0])
    tok_copy.start()

    def w_copies(f):
        return (
            pltpu.make_async_copy(wg_h.at[:, cols(f)], og.at[:, cols(f)], w_sem.at[0, f]),
            pltpu.make_async_copy(wu_h.at[:, cols(f)], ou.at[:, cols(f)], w_sem.at[1, f]),
        )

    for copy in w_copies(0):
        copy.start()
    wd_copy = pltpu.make_async_copy(wd_h, wd, load_sem.at[1])
    tgt_copy = pltpu.make_async_copy(tgt_h.at[mine, :], tg, load_sem.at[2])

    along = lax.rem(g, X)
    last_end = along == X - 1
    first_end = along == 0
    at_end = jnp.logical_or(last_end, first_end)
    layer = g // (X * Y)
    layers = replicas // (X * Y)
    beyond = lax.rem(layer + (along // (X - 1)) * 2 - 1 + layers, layers)
    facing = [
        (at * (X * Y) + row * X + (X - 1 - along), shard)
        for at in (layer, beyond)
        for row in range(Y)
        for shard in range(4)
    ]

    def tell(sem, wheres):
        for where in wheres:
            pl.semaphore_signal(sem, inc=1, device_id=where, device_id_type=MESH)

    barrier = pltpu.get_barrier_semaphore()
    two_away = lax.rem(g + (along // 2) * 4 - 2 + replicas, replicas)
    near = ((g, sibling), (g, peer), (two_away, m))
    inward = g + 1 - 2 * (along // (X - 1))

    @pl.when(jnp.logical_not(at_end))
    def _():
        tell(barrier, (*near, (after, m), (before, m)))

    @pl.when(at_end)
    def _():
        tell(barrier, (*near, (inward, m), *facing))

    tok_copy.wait()
    for f in range(1, n_units):
        for copy in w_copies(f):
            copy.start()
    wd_copy.start()
    tgt_copy.start()

    def norm(i, carry):
        rows = pl.ds(pl.multiple_of(i * 64, 64), 64)
        wide = x[rows, :].astype(F32)
        mean = jnp.mean(wide * wide, axis=-1, keepdims=True)
        nrm[rows, :] = (wide * lax.rsqrt(mean + 1e-06)).astype(BF16)
        return carry

    lax.fori_loop(0, toks // 64, norm, 0)

    def forward(f, carry):
        for copy in w_copies(f):
            copy.wait()
        gate = dot(nrm[...], og[:, cols(f)], ((1,), (0,))) * in_scale
        up = dot(nrm[...], ou[:, cols(f)], ((1,), (0,))) * in_scale
        sig = jax.nn.sigmoid(gate)
        acted = gate * sig
        act[:, cols(f)] = acted
        slope[:, cols(f)] = up * (sig * (1.0 + gate * (1.0 - sig)))
        hid[:, cols(f)] = (acted * up).astype(BF16)
        return carry

    lax.fori_loop(0, n_units, forward, 0)
    wd_copy.wait()

    @pl.when(jnp.logical_not(at_end))
    def _():
        pl.semaphore_wait(barrier, len(near) + 2)

    @pl.when(at_end)
    def _():
        pl.semaphore_wait(barrier, len(near) + 1 + len(facing))

    def p_copy(d):
        return pltpu.make_async_remote_copy(
            src_ref=part.at[theirs, cols(d)], dst_ref=part_in.at[:, cols(d)],
            send_sem=p_send.at[d], recv_sem=p_recv.at[d],
            device_id=(g, sibling), device_id_type=MESH,
        )

    def q_copy(d):
        return pltpu.make_async_remote_copy(
            src_ref=part.at[mine, cols(d)], dst_ref=sum_in.at[:, cols(d)],
            send_sem=q_send.at[d], recv_sem=q_recv.at[d],
            device_id=(g, peer), device_id_type=MESH,
        )

    def e_copy(d):
        return pltpu.make_async_remote_copy(
            src_ref=err.at[mine, cols(d)], dst_ref=err.at[mine, cols(d)],
            send_sem=e_send.at[d], recv_sem=e_recv.at[d],
            device_id=(g, sibling), device_id_type=MESH,
        )

    def pair(src, lo, hi, send, recv, i):
        return (
            pltpu.make_async_remote_copy(
                src_ref=src, dst_ref=lo, send_sem=send.at[0, i], recv_sem=recv.at[0, i],
                device_id=(after, m), device_id_type=MESH,
            ),
            pltpu.make_async_remote_copy(
                src_ref=src, dst_ref=hi, send_sem=send.at[1, i], recv_sem=recv.at[1, i],
                device_id=(before, m), device_id_type=MESH,
            ),
        )

    def d_copies(d):
        return pair(od.at[:, cols(d)], lo_h.at[d], hi_h.at[d], d_send, d_recv, d)

    def g_copies(i):
        rows = cols(i, ROWS)
        return pair(og.at[rows, :], glo.at[rows, :], ghi.at[rows, :], g_send, g_recv, i)

    def u_copies(i):
        rows = cols(i, ROWS)
        return pair(ou.at[rows, :], ulo.at[rows, :], uhi.at[rows, :], u_send, u_recv, i)

    def relay_out():
        return pltpu.make_async_remote_copy(
            src_ref=od.at[:, cols(0)], dst_ref=relay_h,
            send_sem=relay_sem.at[0], recv_sem=relay_sem.at[1],
            device_id=(two_away, m), device_id_type=MESH,
        )

    def relay_on(back):
        dst, where = (lo_h, before) if back else (hi_h, after)
        return pltpu.make_async_remote_copy(
            src_ref=relay_h, dst_ref=dst.at[0],
            send_sem=relay_sem.at[2], recv_sem=d_recv.at[0 if back else 1, 0],
            device_id=(where, m), device_id_type=MESH,
        )

    def partial(d):
        part[:, cols(d)] = dot(hid[...], wd[:, cols(d)], ((1,), (0,))).astype(BF16)
        p_copy(d).start()

    def join(d):
        p_copy(d).wait()
        total = part[mine, cols(d)].astype(F32) + part_in[:, cols(d)].astype(F32)
        part[mine, cols(d)] = total.astype(BF16)
        q_copy(d).start()

    partial(0)
    partial(1)

    def spread(i, carry):
        join(i)
        partial(i + 2)
        return carry

    lax.fori_loop(0, n_cols - 2, spread, 0)
    join(n_cols - 2)
    join(n_cols - 1)

    def turn(i, carry):
        hid_t[cols(i), :] = hid[:, cols(i)].T
        return carry

    lax.fori_loop(0, n_units, turn, 0)
    tgt_copy.wait()

    def down(d, carry):
        q_copy(d).wait()

        @pl.when(jnp.logical_and(at_end, d == n_cols - 1))
        def _():
            tell(go_sem, facing)

        total = part[mine, cols(d)].astype(F32) + sum_in[:, cols(d)].astype(F32)
        offset = x[mine, cols(d)].astype(F32) - tg[:, cols(d)].astype(F32)
        err[mine, cols(d)] = ((offset + total * mid_scale) / toks).astype(BF16)
        e_copy(d).start()
        e_copy(d).wait()
        grad = dot(hid_t[...], err[:, cols(d)], ((1,), (0,)))
        od[:, cols(d)] = (
            wd[:, cols(d)].astype(F32) - (step_size * mid_scale) * grad
        ).astype(BF16)
        ahead, behind = d_copies(d)
        pl.when(jnp.logical_not(last_end))(ahead.start)
        pl.when(jnp.logical_not(first_end))(behind.start)
        pl.when(jnp.logical_and(at_end, d == 0))(relay_out().start)
        return carry

    lax.fori_loop(0, n_cols, down, 0)

    @pl.when(at_end)
    def _():
        pl.semaphore_wait(go_sem, len(facing))

    def held_back(d, carry):
        ahead, behind = d_copies(d)
        pl.when(last_end)(ahead.start)
        pl.when(first_end)(behind.start)
        return carry

    lax.fori_loop(1, n_cols, held_back, 0)

    def back(f, carry):
        grad = dot(err[...], wd[cols(f), :], ((1,), (1,))) * mid_scale
        gg[:, cols(f)] = (grad * slope[:, cols(f)]).astype(BF16)
        gu[:, cols(f)] = (grad * act[:, cols(f)]).astype(BF16)
        return carry

    lax.fori_loop(0, n_units, back, 0)

    def step(out, grads, copies):
        def one(i, carry):
            rows = cols(i, ROWS)
            grad = dot(nrm[:, rows], grads[...], ((0,), (0,)))
            out[rows, :] = (
                out[rows, :].astype(F32) - (step_size * in_scale) * grad
            ).astype(BF16)
            for copy in copies(i):
                copy.start()
            return carry

        lax.fori_loop(0, n_rows, one, 0)

    step(og, gg, g_copies)

    @pl.when(jnp.logical_not(at_end))
    def _():
        relay_out().wait_recv()
        pl.when(along == 1)(relay_on(True).start)
        pl.when(along == 2)(relay_on(False).start)

    step(ou, gu, u_copies)

    def third(lo, own, hi):
        return ((lo.astype(F32) + own.astype(F32) + hi.astype(F32)) / 3.0).astype(BF16)

    def mix_down(i, carry):
        d = lax.rem(i + 1, n_cols)
        ahead, behind = d_copies(d)
        ahead.wait_recv()
        behind.wait_recv()
        relayed = jnp.logical_and(at_end, d == 0)
        pl.when(relayed)(relay_out().wait_send)
        pl.when(jnp.logical_not(jnp.logical_and(last_end, d == 0)))(ahead.wait_send)
        pl.when(jnp.logical_not(jnp.logical_and(first_end, d == 0)))(behind.wait_send)
        loads = [
            pltpu.make_async_copy(lo_h.at[d], stage.at[0], st_sem.at[0]),
            pltpu.make_async_copy(hi_h.at[d], stage.at[1], st_sem.at[1]),
        ]
        for load in loads:
            load.start()
        for load in loads:
            load.wait()
        od[:, cols(d)] = third(stage[0], od[:, cols(d)], stage[1])
        return carry

    lax.fori_loop(0, n_cols, mix_down, 0)

    def mix(out, lo, hi, copies):
        def one(i, carry):
            rows = cols(i, ROWS)
            for copy in copies(i):
                copy.wait()
            out[rows, :] = third(lo[rows, :], out[rows, :], hi[rows, :])
            return carry

        lax.fori_loop(0, n_rows, one, 0)

    pl.when(along == 1)(relay_on(True).wait_send)
    pl.when(along == 2)(relay_on(False).wait_send)
    mix(og, glo, ghi, g_copies)
    mix(ou, ulo, uhi, u_copies)


def write_kernel(pieces, *refs):
    held, out, sem = refs[:3], refs[3:6], refs[6]
    copies = []
    for i in range(3):
        rows = held[i].shape[0] // pieces
        for p in range(pieces):
            part = pl.ds(p * rows, rows)
            copies.append(
                pltpu.make_async_copy(held[i].at[part, :], out[i].at[0, part, :], sem.at[i, p])
            )
    for copy in copies:
        copy.start()
    for copy in copies:
        copy.wait()


def write_out(*arrays):
    pieces = 4
    return pl.pallas_call(
        functools.partial(write_kernel, pieces),
        out_shape=tuple(jax.ShapeDtypeStruct((1, *a.shape), a.dtype) for a in arrays),
        in_specs=[pl.BlockSpec(memory_space=pltpu.VMEM)] * 3,
        out_specs=(pl.BlockSpec(memory_space=pl.ANY),) * 3,
        scratch_shapes=[pltpu.SemaphoreType.DMA((3, pieces))],
        compiler_params=pltpu.CompilerParams(vmem_limit_bytes=16 * 2**20),
    )(*arrays)


def local(replicas, tokens, targets, gate_weight, up_weight, down_weight):
    toks, width = tokens.shape[1:]
    units = gate_weight.shape[2]
    n_cols, n_rows, n_units = width // COLS, width // ROWS, units // COLS
    half = toks // 2
    dma = pltpu.SemaphoreType.DMA
    any_spec = pl.BlockSpec(memory_space=pl.ANY)
    vmem_spec = pl.BlockSpec(memory_space=pltpu.VMEM)
    received = jax.ShapeDtypeStruct((n_cols, units, COLS), BF16)
    gate_out, up_out, down_out, *_ = pl.pallas_call(
        functools.partial(kernel, replicas),
        out_shape=(
            pltpu.VMEM((width, units), BF16),
            pltpu.VMEM((width, units), BF16),
            pltpu.VMEM((units, width), BF16),
            received,
            received,
            jax.ShapeDtypeStruct((units, COLS), BF16),
        ),
        in_specs=[any_spec] * 5,
        out_specs=(vmem_spec, vmem_spec, vmem_spec, any_spec, any_spec, any_spec),
        scratch_shapes=[
            pltpu.VMEM((toks, width), BF16),
            pltpu.VMEM((half, width), BF16),
            pltpu.VMEM((toks, width), BF16),
            pltpu.VMEM((units, width), BF16),
            pltpu.VMEM((toks, units), F32),
            pltpu.VMEM((toks, units), F32),
            pltpu.VMEM((toks, units), BF16),
            pltpu.VMEM((units, toks), BF16),
            pltpu.VMEM((toks, width), BF16),
            pltpu.VMEM((toks, units), BF16),
            pltpu.VMEM((toks, units), BF16),
            pltpu.VMEM((toks, width), BF16),
            pltpu.VMEM((half, width), BF16),
            pltpu.VMEM((half, width), BF16),
            pltpu.VMEM((width, units), BF16),
            pltpu.VMEM((width, units), BF16),
            pltpu.VMEM((width, units), BF16),
            pltpu.VMEM((width, units), BF16),
            pltpu.VMEM((2, units, COLS), BF16),
            dma((3,)),
            dma((2, n_units)),
            dma((n_cols,)),
            dma((n_cols,)),
            dma((n_cols,)),
            dma((n_cols,)),
            dma((n_cols,)),
            dma((n_cols,)),
            dma((2, n_cols)),
            dma((2, n_cols)),
            dma((2, n_rows)),
            dma((2, n_rows)),
            dma((2, n_rows)),
            dma((2, n_rows)),
            dma((2,)),
            dma((3,)),
            pltpu.SemaphoreType.REGULAR,
        ],
        compiler_params=pltpu.CompilerParams(
            collective_id=0, has_side_effects=True, vmem_limit_bytes=50 * 2**20
        ),
    )(tokens[0], targets[0], gate_weight[0], up_weight[0], down_weight[0])
    return write_out(gate_out, up_out, down_out)


def solution(mesh):
    placed = (
        P("gossip", None, None),
        P("gossip", None, None),
        P("gossip", None, "mp"),
        P("gossip", None, "mp"),
        P("gossip", "mp", None),
    )
    return jax.shard_map(
        functools.partial(local, mesh.shape["gossip"]),
        mesh=mesh,
        in_specs=placed,
        out_specs=(P("gossip", None, "mp"), P("gossip", None, "mp"), P("gossip", "mp", None)),
        check_vma=False,
    )
```

```python
import functools

import jax
import jax.numpy as jnp
from jax import lax
from jax.experimental import pallas as pl
from jax.experimental.pallas import tpu as pltpu
from jax.sharding import PartitionSpec as P

MESH = pl.DeviceIdType.MESH
F32 = jnp.float32
BF16 = jnp.bfloat16
COLS = 256
X, Y = 4, 2
ROWS = 256
REST = 304
AWAY = 224
FIRST = 128


def dot(a, b, dims):
    return lax.dot_general(a, b, (dims, ((), ())), preferred_element_type=F32)


def kernel(
    replicas,
    tok_h, tgt_h, wg_h, wu_h, wd_h,
    og, ou, od, lo_h, hi_h, relay_h,
    x, tg, inv, nrm, wd, slope, act, hid, hid_t, err, gg, gu,
    part, part_in, sum_in, glo, ghi, ulo, uhi, stage, crossing, summing,
    tok_sem, load_sem, w_sem, p_send, p_recv, q_send, q_recv, e_send, e_recv,
    d_send, d_recv, g_send, g_recv, u_send, u_recv, st_sem,
    b_send, b_recv, relay_sem, cross_sem, go_sem,
):
    g = lax.axis_index("gossip")
    m = lax.axis_index("mp")
    core = lax.rem(m, 2)
    sibling = m + 1 - 2 * core
    peer = lax.rem(m + 2, 4)
    after = lax.rem(g + 1, replicas)
    before = lax.rem(g + replicas - 1, replicas)
    toks, width = x.shape
    units = wd.shape[0]
    half = toks // 2
    in_scale = 1.0 / width**0.5
    mid_scale = 1.0 / (4 * units) ** 0.5
    step_size = (4 * units) / 4.0

    def cols(i, size=COLS):
        return pl.ds(pl.multiple_of(i * size, size), size)

    n_cols = width // COLS
    n_rows = width // ROWS
    n_rest = (width - AWAY) // REST
    rows_b = pl.ds(0, AWAY)
    early, late = pl.ds(0, FIRST), pl.ds(FIRST, COLS - FIRST)
    n_units = units // COLS
    mine = pl.ds(pl.multiple_of(core * half, half), half)
    theirs = pl.ds(pl.multiple_of((1 - core) * half, half), half)

    piece = toks // 4

    def tok_copy(i):
        rows = cols(i, piece)
        return pltpu.make_async_copy(tok_h.at[rows, :], x.at[rows, :], tok_sem.at[i])

    for i in range(4):
        tok_copy(i).start()

    def w_copies(f):
        return (
            pltpu.make_async_copy(wg_h.at[:, cols(f)], og.at[:, cols(f)], w_sem.at[0, f]),
            pltpu.make_async_copy(wu_h.at[:, cols(f)], ou.at[:, cols(f)], w_sem.at[1, f]),
        )

    for copy in w_copies(0):
        copy.start()

    wd_copy = pltpu.make_async_copy(wd_h, wd, load_sem.at[0])
    tgt_copy = pltpu.make_async_copy(tgt_h.at[mine, :], tg, load_sem.at[1])

    along = lax.rem(g, X)
    last_end = along == X - 1
    first_end = along == 0
    at_end = jnp.logical_or(last_end, first_end)
    layer = g // (X * Y)
    layers = replicas // (X * Y)
    beyond = lax.rem(layer + (along // (X - 1)) * 2 - 1 + layers, layers)
    facing = [
        (at * (X * Y) + row * X + (X - 1 - along), shard)
        for at in (layer, beyond)
        for row in range(Y)
        for shard in range(4)
    ]

    def tell(sem, wheres):
        for where in wheres:
            pl.semaphore_signal(sem, inc=1, device_id=where, device_id_type=MESH)

    barrier = pltpu.get_barrier_semaphore()
    far_end = g + (X - 1) * (1 - 2 * (along // (X - 1)))
    diagonal = lax.rem(g + (X + 1) * (1 - 2 * lax.rem(along, 2)) + replicas, replicas)
    across_up = lax.rem(g + X, replicas)
    across_down = lax.rem(g - X + replicas, replicas)
    near = ((g, sibling), (g, peer), (diagonal, m))
    inward = g + 1 - 2 * (along // (X - 1))

    @pl.when(jnp.logical_not(at_end))
    def _():
        tell(barrier, (*near, (after, m), (before, m), (across_up, m), (across_down, m)))

    @pl.when(at_end)
    def _():
        tell(barrier, (*near, (inward, m), *facing))

    def square(i, carry):
        rows = cols(i, 64)
        wide = x[rows, :].astype(F32)
        mean = jnp.mean(wide * wide, axis=-1, keepdims=True)
        inv[rows, :] = lax.rsqrt(mean + 1e-06)
        return carry

    for i in range(4):
        tok_copy(i).wait()
        lax.fori_loop(i * piece // 64, (i + 1) * piece // 64, square, 0)
        for copy in w_copies(i + 1) if i + 1 < n_units else (wd_copy, tgt_copy):
            copy.start()

    def forward(f, carry):
        for copy in w_copies(f):
            copy.wait()
        scale = inv[...] * in_scale
        gate = dot(x[...], og[:, cols(f)], ((1,), (0,))) * scale
        up = dot(x[...], ou[:, cols(f)], ((1,), (0,))) * scale
        sig = jax.nn.sigmoid(gate)
        acted = gate * sig
        act[:, cols(f)] = acted
        slope[:, cols(f)] = up * (sig * (1.0 + gate * (1.0 - sig)))
        hid[:, cols(f)] = (acted * up).astype(BF16)
        return carry

    lax.fori_loop(0, n_units, forward, 0)
    wd_copy.wait()

    @pl.when(jnp.logical_not(at_end))
    def _():
        pl.semaphore_wait(barrier, len(near) + 4)

    @pl.when(at_end)
    def _():
        pl.semaphore_wait(barrier, len(near) + 1 + len(facing))

    def p_copy(d):
        return pltpu.make_async_remote_copy(
            src_ref=part.at[theirs, cols(d)], dst_ref=part_in.at[:, cols(d)],
            send_sem=p_send.at[d], recv_sem=p_recv.at[d],
            device_id=(g, sibling), device_id_type=MESH,
        )

    def q_copy(d):
        return pltpu.make_async_remote_copy(
            src_ref=part.at[mine, cols(d)], dst_ref=sum_in.at[:, cols(d)],
            send_sem=q_send.at[d], recv_sem=q_recv.at[d],
            device_id=(g, peer), device_id_type=MESH,
        )

    def e_copy(d):
        return pltpu.make_async_remote_copy(
            src_ref=err.at[mine, cols(d)], dst_ref=err.at[mine, cols(d)],
            send_sem=e_send.at[d], recv_sem=e_recv.at[d],
            device_id=(g, sibling), device_id_type=MESH,
        )

    def pair(src, lo, hi, send, recv, i):
        def sem(sems, k):
            return sems.at[k] if i is None else sems.at[k, i]

        return (
            pltpu.make_async_remote_copy(
                src_ref=src, dst_ref=lo, send_sem=sem(send, 0), recv_sem=sem(recv, 0),
                device_id=(after, m), device_id_type=MESH,
            ),
            pltpu.make_async_remote_copy(
                src_ref=src, dst_ref=hi, send_sem=sem(send, 1), recv_sem=sem(recv, 1),
                device_id=(before, m), device_id_type=MESH,
            ),
        )

    def d_copies(d):
        return pair(od.at[:, cols(d)], lo_h.at[d], hi_h.at[d], d_send, d_recv, d)

    def g_pair(rows, send, recv, i):
        return pair(og.at[rows, :], glo.at[rows, :], ghi.at[rows, :], send, recv, i)

    def rest(i):
        return pl.ds(pl.multiple_of(AWAY + i * REST, 16), REST)

    def g_copies(i):
        return g_pair(rest(i), g_send, g_recv, i)

    def b_copies():
        return g_pair(rows_b, b_send, b_recv, None)

    def u_copies(i):
        rows = cols(i, ROWS)
        return pair(ou.at[rows, :], ulo.at[rows, :], uhi.at[rows, :], u_send, u_recv, i)

    def send(src, dst, send_sem, recv_sem, replica):
        return pltpu.make_async_remote_copy(
            src_ref=src, dst_ref=dst, send_sem=send_sem, recv_sem=recv_sem,
            device_id=(replica, m), device_id_type=MESH,
        )

    def relay_out():
        return send(od.at[:, early], relay_h, relay_sem.at[0], relay_sem.at[1], far_end)

    def relay_over():
        return send(relay_h, relay_h, relay_sem.at[2], relay_sem.at[1], diagonal)

    def relay_on(first):
        dst, k, where = (lo_h, 0, before) if first else (hi_h, 1, after)
        return send(relay_h, dst.at[0, :, early], relay_sem.at[2], d_recv.at[k, 0], where)

    def late_copies():
        return (
            send(od.at[:, late], lo_h.at[0, :, late], d_send.at[0, 0], d_recv.at[0, 0], after),
            send(od.at[:, late], hi_h.at[0, :, late], d_send.at[1, 0], d_recv.at[1, 0], before),
        )

    def cross_out(first):
        src, where = (glo, across_down) if first else (ghi, across_up)
        return send(src.at[rows_b, :], crossing, cross_sem.at[0], cross_sem.at[1], where)

    def cross_in(first):
        return send(crossing, summing, cross_sem.at[2], cross_sem.at[3], after if first else before)

    def cross_end(first):
        dst, where = (ghi, before) if first else (glo, after)
        return send(summing, dst.at[rows_b, :], cross_sem.at[4], cross_sem.at[5], where)

    def partial(d):
        part[:, cols(d)] = dot(hid[...], wd[:, cols(d)], ((1,), (0,))).astype(BF16)
        p_copy(d).start()

    def join(d):
        p_copy(d).wait()
        total = part[mine, cols(d)].astype(F32) + part_in[:, cols(d)].astype(F32)
        part[mine, cols(d)] = total.astype(BF16)
        q_copy(d).start()

    partial(0)
    partial(1)

    def spread(i, carry):
        join(i)
        partial(i + 2)
        return carry

    lax.fori_loop(0, n_cols - 2, spread, 0)
    join(n_cols - 2)
    join(n_cols - 1)

    def turn(i, carry):
        hid_t[cols(i), :] = hid[:, cols(i)].T
        return carry

    lax.fori_loop(0, n_units, turn, 0)

    def norm(i, carry):
        rows = cols(i, 64)
        nrm[rows, :] = (x[rows, :].astype(F32) * inv[rows, :]).astype(BF16)
        return carry

    lax.fori_loop(0, toks // 64, norm, 0)
    tgt_copy.wait()

    def down(d, carry):
        q_copy(d).wait()

        @pl.when(jnp.logical_and(at_end, d == n_cols - 1))
        def _():
            tell(go_sem, facing)

        total = part[mine, cols(d)].astype(F32) + sum_in[:, cols(d)].astype(F32)
        offset = x[mine, cols(d)].astype(F32) - tg[:, cols(d)].astype(F32)
        err[mine, cols(d)] = ((offset + total * mid_scale) / toks).astype(BF16)
        e_copy(d).start()
        e_copy(d).wait()
        grad = dot(hid_t[...], err[:, cols(d)], ((1,), (0,)))
        od[:, cols(d)] = (
            wd[:, cols(d)].astype(F32) - (step_size * mid_scale) * grad
        ).astype(BF16)
        ahead, behind = d_copies(d)
        pl.when(jnp.logical_not(last_end))(ahead.start)
        pl.when(jnp.logical_not(first_end))(behind.start)
        pl.when(jnp.logical_and(at_end, d == 0))(relay_out().start)
        return carry

    lax.fori_loop(0, n_cols, down, 0)

    @pl.when(at_end)
    def _():
        pl.semaphore_wait(go_sem, len(facing))

    def held_back(d, carry):
        ahead, behind = d_copies(d)
        pl.when(last_end)(ahead.start)
        pl.when(first_end)(behind.start)
        return carry

    ahead, behind = late_copies()
    pl.when(last_end)(ahead.start)
    pl.when(first_end)(behind.start)
    lax.fori_loop(1, n_cols, held_back, 0)

    def back(f, carry):
        grad = dot(err[...], wd[cols(f), :], ((1,), (1,))) * mid_scale
        gg[:, cols(f)] = (grad * slope[:, cols(f)]).astype(BF16)
        gu[:, cols(f)] = (grad * act[:, cols(f)]).astype(BF16)
        return carry

    lax.fori_loop(0, n_units, back, 0)

    @pl.when(at_end)
    def _():
        relay_out().wait_recv()
        relay_over().start()

    def step(out, grads, rows):
        grad = dot(nrm[:, rows], grads[...], ((0,), (0,)))
        out[rows, :] = (out[rows, :].astype(F32) - (step_size * in_scale) * grad).astype(BF16)

    def step_up(i, carry):
        step(ou, gu, cols(i, ROWS))
        return carry

    def send_up(i, carry):
        for copy in u_copies(i):
            copy.start()
        return carry

    lower, upper = along <= 1, along >= 2
    inside = jnp.logical_not(at_end)
    first_in, last_in = along == 1, along == 2

    def step_gate(i, carry):
        step(og, gg, pl.ds(pl.multiple_of(i * 128, 128), 128))
        return carry

    def send_gate(i, carry):
        for copy in g_copies(i):
            copy.start()
        return carry

    lax.fori_loop(0, width // 128, step_gate, 0)
    ahead, behind = b_copies()
    pl.when(lower)(ahead.start)
    pl.when(upper)(behind.start)
    lax.fori_loop(0, n_rest, send_gate, 0)
    lax.fori_loop(0, n_rows, step_up, 0)

    def third(lo, own, hi):
        return ((lo.astype(F32) + own.astype(F32) + hi.astype(F32)) / 3.0).astype(BF16)

    def mix_down(d, carry):
        ahead, behind = d_copies(d)
        ahead.wait_recv()
        behind.wait_recv()
        pl.when(jnp.logical_not(jnp.logical_and(last_end, d == 0)))(ahead.wait_send)
        pl.when(jnp.logical_not(jnp.logical_and(first_end, d == 0)))(behind.wait_send)
        ahead, behind = late_copies()
        pl.when(jnp.logical_and(last_end, d == 0))(ahead.wait_send)
        pl.when(jnp.logical_and(first_end, d == 0))(behind.wait_send)
        pl.when(jnp.logical_and(at_end, d == 0))(relay_out().wait_send)
        loads = [
            pltpu.make_async_copy(lo_h.at[d], stage.at[0], st_sem.at[0]),
            pltpu.make_async_copy(hi_h.at[d], stage.at[1], st_sem.at[1]),
        ]
        for load in loads:
            load.start()
        for load in loads:
            load.wait()
        od[:, cols(d)] = third(stage[0], od[:, cols(d)], stage[1])
        return carry

    lax.fori_loop(1, n_cols, mix_down, 0)

    @pl.when(inside)
    def _():
        relay_out().wait_recv()
        pl.when(first_in)(relay_on(True).start)
        pl.when(last_in)(relay_on(False).start)
        for copy in b_copies():
            copy.wait_recv()
        pl.when(first_in)(cross_out(True).start)
        pl.when(last_in)(cross_out(False).start)
        cross_out(True).wait_recv()
        pl.when(first_in)(cross_in(True).start)
        pl.when(last_in)(cross_in(False).start)

    lax.fori_loop(0, n_rows, send_up, 0)

    def mix(out, lo, hi, rows):
        out[rows, :] = third(lo[rows, :], out[rows, :], hi[rows, :])

    def mix_gate(i, carry):
        for copy in g_copies(i):
            copy.wait()
        mix(og, glo, ghi, rest(i))
        return carry

    lax.fori_loop(0, n_rest, mix_gate, 0)
    lax.fori_loop(0, 1, mix_down, 0)
    ahead, behind = b_copies()
    pl.when(lower)(ahead.wait_send)
    pl.when(upper)(behind.wait_send)

    @pl.when(inside)
    def _():
        cross_in(True).wait_recv()
        both = summing[...].astype(F32) + og[rows_b, :].astype(F32)
        summing[...] = both.astype(BF16)
        pl.when(first_in)(cross_end(True).start)
        pl.when(last_in)(cross_end(False).start)
        cross_out(True).wait_send()
        mix(og, glo, ghi, rows_b)

    def mix_up(i, carry):
        for copy in u_copies(i):
            copy.wait()
        mix(ou, ulo, uhi, cols(i, ROWS))
        return carry

    lax.fori_loop(0, n_rows, mix_up, 0)

    def end(own, both):
        return ((own.astype(F32) + both.astype(F32)) / 3.0).astype(BF16)

    relay_over().wait_send()

    @pl.when(inside)
    def _():
        cross_in(True).wait_send()
        cross_end(True).wait_send()

    @pl.when(first_end)
    def _():
        cross_end(True).wait_recv()
        og[rows_b, :] = end(og[rows_b, :], ghi[rows_b, :])

    @pl.when(last_end)
    def _():
        cross_end(False).wait_recv()
        og[rows_b, :] = end(og[rows_b, :], glo[rows_b, :])


def write_kernel(pieces, *refs):
    held, out, sem = refs[:3], refs[3:6], refs[6]
    copies = []
    for i in range(3):
        rows = held[i].shape[0] // pieces
        for p in range(pieces):
            part = pl.ds(p * rows, rows)
            copies.append(
                pltpu.make_async_copy(held[i].at[part, :], out[i].at[0, part, :], sem.at[i, p])
            )
    for copy in copies:
        copy.start()
    for copy in copies:
        copy.wait()


def write_out(*arrays):
    pieces = 4
    return pl.pallas_call(
        functools.partial(write_kernel, pieces),
        out_shape=tuple(jax.ShapeDtypeStruct((1, *a.shape), a.dtype) for a in arrays),
        in_specs=[pl.BlockSpec(memory_space=pltpu.VMEM)] * 3,
        out_specs=(pl.BlockSpec(memory_space=pl.ANY),) * 3,
        scratch_shapes=[pltpu.SemaphoreType.DMA((3, pieces))],
        compiler_params=pltpu.CompilerParams(vmem_limit_bytes=16 * 2**20),
    )(*arrays)


def local(replicas, tokens, targets, gate_weight, up_weight, down_weight):
    toks, width = tokens.shape[1:]
    units = gate_weight.shape[2]
    n_cols, n_rows, n_units = width // COLS, width // ROWS, units // COLS
    n_rest = (width - AWAY) // REST
    half = toks // 2
    dma = pltpu.SemaphoreType.DMA
    any_spec = pl.BlockSpec(memory_space=pl.ANY)
    vmem_spec = pl.BlockSpec(memory_space=pltpu.VMEM)
    received = jax.ShapeDtypeStruct((n_cols, units, COLS), BF16)
    gate_out, up_out, down_out, *_ = pl.pallas_call(
        functools.partial(kernel, replicas),
        out_shape=(
            pltpu.VMEM((width, units), BF16),
            pltpu.VMEM((width, units), BF16),
            pltpu.VMEM((units, width), BF16),
            received,
            received,
            jax.ShapeDtypeStruct((units, FIRST), BF16),
        ),
        in_specs=[any_spec] * 5,
        out_specs=(vmem_spec, vmem_spec, vmem_spec, any_spec, any_spec, any_spec),
        scratch_shapes=[
            pltpu.VMEM((toks, width), BF16),
            pltpu.VMEM((half, width), BF16),
            pltpu.VMEM((toks, 1), F32),
            pltpu.VMEM((toks, width), BF16),
            pltpu.VMEM((units, width), BF16),
            pltpu.VMEM((toks, units), F32),
            pltpu.VMEM((toks, units), F32),
            pltpu.VMEM((toks, units), BF16),
            pltpu.VMEM((units, toks), BF16),
            pltpu.VMEM((toks, width), BF16),
            pltpu.VMEM((toks, units), BF16),
            pltpu.VMEM((toks, units), BF16),
            pltpu.VMEM((toks, width), BF16),
            pltpu.VMEM((half, width), BF16),
            pltpu.VMEM((half, width), BF16),
            pltpu.VMEM((width, units), BF16),
            pltpu.VMEM((width, units), BF16),
            pltpu.VMEM((width, units), BF16),
            pltpu.VMEM((width, units), BF16),
            pltpu.VMEM((2, units, COLS), BF16),
            pltpu.VMEM((AWAY, units), BF16),
            pltpu.VMEM((AWAY, units), BF16),
            dma((4,)),
            dma((2,)),
            dma((2, n_units)),
            dma((n_cols,)),
            dma((n_cols,)),
            dma((n_cols,)),
            dma((n_cols,)),
            dma((n_cols,)),
            dma((n_cols,)),
            dma((2, n_cols)),
            dma((2, n_cols)),
            dma((2, n_rest)),
            dma((2, n_rest)),
            dma((2, n_rows)),
            dma((2, n_rows)),
            dma((2,)),
            dma((2,)),
            dma((2,)),
            dma((3,)),
            dma((6,)),
            pltpu.SemaphoreType.REGULAR,
        ],
        compiler_params=pltpu.CompilerParams(
            collective_id=0, has_side_effects=True, vmem_limit_bytes=50 * 2**20
        ),
    )(tokens[0], targets[0], gate_weight[0], up_weight[0], down_weight[0])
    return write_out(gate_out, up_out, down_out)


def solution(mesh):
    placed = (
        P("gossip", None, None),
        P("gossip", None, None),
        P("gossip", None, "mp"),
        P("gossip", None, "mp"),
        P("gossip", "mp", None),
    )
    return jax.shard_map(
        functools.partial(local, mesh.shape["gossip"]),
        mesh=mesh,
        in_specs=placed,
        out_specs=(P("gossip", None, "mp"), P("gossip", None, "mp"), P("gossip", "mp", None)),
        check_vma=False,
    )
```

```python
import functools

import jax
import jax.numpy as jnp
from jax import lax
from jax.experimental import pallas as pl
from jax.experimental.pallas import tpu as pltpu
from jax.sharding import PartitionSpec as P

MESH = pl.DeviceIdType.MESH
F32 = jnp.float32
BF16 = jnp.bfloat16
COLS = 256
X, Y = 4, 2
ROWS = 256
REST = 368
AWAY = 208
FIRST = 768
HEAD = 128


def dot(a, b, dims):
    return lax.dot_general(a, b, (dims, ((), ())), preferred_element_type=F32)


def kernel(
    replicas,
    tok_h, tgt_h, wg_h, wu_h, wd_h,
    og, ou, od, lo_h, hi_h, relay_h,
    x, tg, inv, nrm, wd, slope, act, hid, hid_t, err, gg, gu,
    part, part_in, sum_in, glo, ghi, ulo, uhi, stage, crossing, summing,
    tok_sem, load_sem, w_sem, p_send, p_recv, q_send, q_recv, e_send, e_recv,
    d_send, d_recv, g_send, g_recv, u_send, u_recv, st_sem,
    b_send, b_recv, relay_sem, cross_sem, go_sem,
):
    g = lax.axis_index("gossip")
    m = lax.axis_index("mp")
    core = lax.rem(m, 2)
    sibling = m + 1 - 2 * core
    peer = lax.rem(m + 2, 4)
    after = lax.rem(g + 1, replicas)
    before = lax.rem(g + replicas - 1, replicas)
    toks, width = x.shape
    units = wd.shape[0]
    half = toks // 2
    in_scale = 1.0 / width**0.5
    mid_scale = 1.0 / (4 * units) ** 0.5
    step_size = (4 * units) / 4.0

    def cols(i, size=COLS):
        return pl.ds(pl.multiple_of(i * size, size), size)

    n_cols = width // COLS
    n_rows = width // ROWS
    n_rest = (width - AWAY) // REST
    rows_b = pl.ds(0, AWAY)
    early, late = pl.ds(0, FIRST), pl.ds(FIRST, units - FIRST)
    n_units = units // COLS
    mine = pl.ds(pl.multiple_of(core * half, half), half)
    theirs = pl.ds(pl.multiple_of((1 - core) * half, half), half)

    piece = toks // 4

    def tok_copy(i):
        rows = cols(i, piece)
        return pltpu.make_async_copy(tok_h.at[rows, :], x.at[rows, :], tok_sem.at[i])

    for i in range(4):
        tok_copy(i).start()

    def w_copies(f):
        return (
            pltpu.make_async_copy(wg_h.at[:, cols(f)], og.at[:, cols(f)], w_sem.at[0, f]),
            pltpu.make_async_copy(wu_h.at[:, cols(f)], ou.at[:, cols(f)], w_sem.at[1, f]),
        )

    for copy in w_copies(0):
        copy.start()

    wd_copy = pltpu.make_async_copy(wd_h, wd, load_sem.at[0])
    tgt_copy = pltpu.make_async_copy(tgt_h.at[mine, :], tg, load_sem.at[1])

    along = lax.rem(g, X)
    last_end = along == X - 1
    first_end = along == 0
    at_end = jnp.logical_or(last_end, first_end)
    layer = g // (X * Y)
    layers = replicas // (X * Y)
    beyond = lax.rem(layer + (along // (X - 1)) * 2 - 1 + layers, layers)
    facing = [
        (at * (X * Y) + row * X + (X - 1 - along), shard)
        for at in (layer, beyond)
        for row in range(Y)
        for shard in range(4)
    ]

    def tell(sem, wheres):
        for where in wheres:
            pl.semaphore_signal(sem, inc=1, device_id=where, device_id_type=MESH)

    barrier = pltpu.get_barrier_semaphore()
    far_end = g + (X - 1) * (1 - 2 * (along // (X - 1)))
    diagonal = lax.rem(g + (X + 1) * (1 - 2 * lax.rem(along, 2)) + replicas, replicas)
    across_up = lax.rem(g + X, replicas)
    across_down = lax.rem(g - X + replicas, replicas)
    near = ((g, sibling), (g, peer), (diagonal, m))
    inward = g + 1 - 2 * (along // (X - 1))

    @pl.when(jnp.logical_not(at_end))
    def _():
        tell(barrier, (*near, (after, m), (before, m), (across_up, m), (across_down, m)))

    @pl.when(at_end)
    def _():
        tell(barrier, (*near, (inward, m), *facing))

    def square(i, carry):
        rows = cols(i, 64)
        wide = x[rows, :].astype(F32)
        mean = jnp.mean(wide * wide, axis=-1, keepdims=True)
        inv[rows, :] = lax.rsqrt(mean + 1e-06)
        return carry

    for i in range(4):
        tok_copy(i).wait()
        lax.fori_loop(i * piece // 64, (i + 1) * piece // 64, square, 0)
        for copy in w_copies(i + 1) if i + 1 < n_units else (wd_copy, tgt_copy):
            copy.start()

    def forward(f, carry):
        for copy in w_copies(f):
            copy.wait()
        scale = inv[...] * in_scale
        gate = dot(x[...], og[:, cols(f)], ((1,), (0,))) * scale
        up = dot(x[...], ou[:, cols(f)], ((1,), (0,))) * scale
        sig = jax.nn.sigmoid(gate)
        acted = gate * sig
        act[:, cols(f)] = acted
        slope[:, cols(f)] = up * (sig * (1.0 + gate * (1.0 - sig)))
        hid[:, cols(f)] = (acted * up).astype(BF16)
        return carry

    lax.fori_loop(0, n_units, forward, 0)
    wd_copy.wait()

    @pl.when(jnp.logical_not(at_end))
    def _():
        pl.semaphore_wait(barrier, len(near) + 4)

    @pl.when(at_end)
    def _():
        pl.semaphore_wait(barrier, len(near) + 1 + len(facing))

    def p_copy(at, k):
        return pltpu.make_async_remote_copy(
            src_ref=part.at[theirs, at], dst_ref=part_in.at[:, at],
            send_sem=p_send.at[k], recv_sem=p_recv.at[k],
            device_id=(g, sibling), device_id_type=MESH,
        )

    def q_copy(at, k):
        return pltpu.make_async_remote_copy(
            src_ref=part.at[mine, at], dst_ref=sum_in.at[:, at],
            send_sem=q_send.at[k], recv_sem=q_recv.at[k],
            device_id=(g, peer), device_id_type=MESH,
        )

    def e_copy(at, k):
        return pltpu.make_async_remote_copy(
            src_ref=err.at[mine, at], dst_ref=err.at[mine, at],
            send_sem=e_send.at[k], recv_sem=e_recv.at[k],
            device_id=(g, sibling), device_id_type=MESH,
        )

    def pair(src, lo, hi, send, recv, i):
        def sem(sems, k):
            return sems.at[k] if i is None else sems.at[k, i]

        return (
            pltpu.make_async_remote_copy(
                src_ref=src, dst_ref=lo, send_sem=sem(send, 0), recv_sem=sem(recv, 0),
                device_id=(after, m), device_id_type=MESH,
            ),
            pltpu.make_async_remote_copy(
                src_ref=src, dst_ref=hi, send_sem=sem(send, 1), recv_sem=sem(recv, 1),
                device_id=(before, m), device_id_type=MESH,
            ),
        )

    def d_copies(d):
        return pair(od.at[:, cols(d)], lo_h.at[d], hi_h.at[d], d_send, d_recv, d)

    def g_pair(rows, send, recv, i):
        return pair(og.at[rows, :], glo.at[rows, :], ghi.at[rows, :], send, recv, i)

    def rest(i):
        return pl.ds(pl.multiple_of(AWAY + i * REST, 16), REST)

    def g_copies(i):
        return g_pair(rest(i), g_send, g_recv, i)

    def b_copies():
        return g_pair(rows_b, b_send, b_recv, None)

    def u_copies(i):
        rows = cols(i, ROWS)
        return pair(ou.at[rows, :], ulo.at[rows, :], uhi.at[rows, :], u_send, u_recv, i)

    def send(src, dst, send_sem, recv_sem, replica):
        return pltpu.make_async_remote_copy(
            src_ref=src, dst_ref=dst, send_sem=send_sem, recv_sem=recv_sem,
            device_id=(replica, m), device_id_type=MESH,
        )

    def relay_out():
        return send(od.at[early, cols(0)], relay_h, relay_sem.at[0], relay_sem.at[1], far_end)

    def relay_over():
        return send(relay_h, relay_h, relay_sem.at[2], relay_sem.at[1], diagonal)

    def relay_on(first):
        dst, k, where = (lo_h, 0, before) if first else (hi_h, 1, after)
        return send(relay_h, dst.at[0, early, :], relay_sem.at[2], d_recv.at[k, 0], where)

    def late_copies():
        return (
            send(od.at[late, cols(0)], lo_h.at[0, late, :], d_send.at[0, 0], d_recv.at[0, 0], after),
            send(od.at[late, cols(0)], hi_h.at[0, late, :], d_send.at[1, 0], d_recv.at[1, 0], before),
        )

    def cross_out(first):
        src, where = (glo, across_down) if first else (ghi, across_up)
        return send(src.at[rows_b, :], crossing, cross_sem.at[0], cross_sem.at[1], where)

    def cross_in(first):
        return send(crossing, summing, cross_sem.at[2], cross_sem.at[3], after if first else before)

    def cross_end(first):
        dst, where = (ghi, before) if first else (glo, after)
        return send(summing, dst.at[rows_b, :], cross_sem.at[4], cross_sem.at[5], where)

    def head(i):
        return cols(i, HEAD), i

    def block(d):
        return cols(d), d + COLS // HEAD - 1

    n_heads = COLS // HEAD
    last = n_cols + n_heads - 2

    def partial(d, carry):
        part[:, cols(d)] = dot(hid[...], wd[:, cols(d)], ((1,), (0,))).astype(BF16)

        @pl.when(d == 0)
        def _():
            for i in range(n_heads):
                p_copy(*head(i)).start()

        pl.when(d > 0)(p_copy(*block(d)).start)
        return carry

    def join(at, k):
        p_copy(at, k).wait()
        total = part[mine, at].astype(F32) + part_in[:, at].astype(F32)
        part[mine, at] = total.astype(BF16)
        q_copy(at, k).start()

    def join_head(i, carry):
        join(*head(i))
        return carry

    def spread(d, carry):
        partial(d, carry)
        join(*block(d - 1))
        return carry

    lax.fori_loop(0, 2, partial, 0)
    lax.fori_loop(0, n_heads, join_head, 0)
    lax.fori_loop(2, n_cols, spread, 0)
    join(*block(n_cols - 1))

    def turn(i, carry):
        hid_t[cols(i), :] = hid[:, cols(i)].T
        return carry

    lax.fori_loop(0, n_units, turn, 0)

    def norm(i, carry):
        rows = cols(i, 64)
        nrm[rows, :] = (x[rows, :].astype(F32) * inv[rows, :]).astype(BF16)
        return carry

    lax.fori_loop(0, toks // 64, norm, 0)
    tgt_copy.wait()

    def step_down(at, k):
        q_copy(at, k).wait()

        @pl.when(jnp.logical_and(at_end, k == last))
        def _():
            tell(go_sem, facing)

        total = part[mine, at].astype(F32) + sum_in[:, at].astype(F32)
        offset = x[mine, at].astype(F32) - tg[:, at].astype(F32)
        err[mine, at] = ((offset + total * mid_scale) / toks).astype(BF16)
        e_copy(at, k).start()
        e_copy(at, k).wait()
        grad = dot(hid_t[...], err[:, at], ((1,), (0,)))
        od[:, at] = (wd[:, at].astype(F32) - (step_size * mid_scale) * grad).astype(BF16)

    def inward_start(ahead, behind):
        pl.when(jnp.logical_not(last_end))(ahead.start)
        pl.when(jnp.logical_not(first_end))(behind.start)

    def down_head(i, carry):
        at, k = head(i)
        step_down(at, k)
        inward_start(
            *pair(od.at[:, at], lo_h.at[0, :, at], hi_h.at[0, :, at], d_send, d_recv, 0)
        )
        return carry

    def down(d, carry):
        step_down(*block(d))
        inward_start(*d_copies(d))
        return carry

    lax.fori_loop(0, n_heads, down_head, 0)
    pl.when(at_end)(relay_out().start)
    lax.fori_loop(1, n_cols, down, 0)

    @pl.when(at_end)
    def _():
        pl.semaphore_wait(go_sem, len(facing))

    def held_back(d, carry):
        ahead, behind = d_copies(d)
        pl.when(last_end)(ahead.start)
        pl.when(first_end)(behind.start)
        return carry

    ahead, behind = late_copies()
    pl.when(last_end)(ahead.start)
    pl.when(first_end)(behind.start)
    lax.fori_loop(1, n_cols, held_back, 0)

    def back(f, carry):
        grad = dot(err[...], wd[cols(f), :], ((1,), (1,))) * mid_scale
        gg[:, cols(f)] = (grad * slope[:, cols(f)]).astype(BF16)
        gu[:, cols(f)] = (grad * act[:, cols(f)]).astype(BF16)
        return carry

    lax.fori_loop(0, n_units, back, 0)

    @pl.when(at_end)
    def _():
        relay_out().wait_recv()
        relay_over().start()

    def step(out, grads, rows):
        grad = dot(nrm[:, rows], grads[...], ((0,), (0,)))
        out[rows, :] = (out[rows, :].astype(F32) - (step_size * in_scale) * grad).astype(BF16)

    def step_up(i, carry):
        step(ou, gu, cols(i, ROWS))
        return carry

    def send_up(i, carry):
        for copy in u_copies(i):
            copy.start()
        return carry

    lower, upper = along <= 1, along >= 2
    inside = jnp.logical_not(at_end)
    first_in, last_in = along == 1, along == 2

    def step_gate(i, carry):
        step(og, gg, pl.ds(pl.multiple_of(i * 128, 128), 128))
        return carry

    def send_gate(i, carry):
        for copy in g_copies(i):
            copy.start()
        return carry

    lax.fori_loop(0, width // 128, step_gate, 0)
    ahead, behind = b_copies()
    pl.when(lower)(ahead.start)
    pl.when(upper)(behind.start)
    lax.fori_loop(0, n_rest, send_gate, 0)
    lax.fori_loop(0, n_rows, step_up, 0)

    def third(lo, own, hi):
        return ((lo.astype(F32) + own.astype(F32) + hi.astype(F32)) / 3.0).astype(BF16)

    def mix_down(d, carry):
        ahead, behind = d_copies(d)
        ahead.wait_recv()
        behind.wait_recv()
        pl.when(jnp.logical_not(jnp.logical_and(last_end, d == 0)))(ahead.wait_send)
        pl.when(jnp.logical_not(jnp.logical_and(first_end, d == 0)))(behind.wait_send)
        ahead, behind = late_copies()
        pl.when(jnp.logical_and(last_end, d == 0))(ahead.wait_send)
        pl.when(jnp.logical_and(first_end, d == 0))(behind.wait_send)
        pl.when(jnp.logical_and(at_end, d == 0))(relay_out().wait_send)
        loads = [
            pltpu.make_async_copy(lo_h.at[d], stage.at[0], st_sem.at[0]),
            pltpu.make_async_copy(hi_h.at[d], stage.at[1], st_sem.at[1]),
        ]
        for load in loads:
            load.start()
        for load in loads:
            load.wait()
        od[:, cols(d)] = third(stage[0], od[:, cols(d)], stage[1])
        return carry

    lax.fori_loop(1, n_cols, mix_down, 0)

    @pl.when(inside)
    def _():
        relay_out().wait_recv()
        pl.when(first_in)(relay_on(True).start)
        pl.when(last_in)(relay_on(False).start)
        for copy in b_copies():
            copy.wait_recv()
        pl.when(first_in)(cross_out(True).start)
        pl.when(last_in)(cross_out(False).start)
        cross_out(True).wait_recv()
        pl.when(first_in)(cross_in(True).start)
        pl.when(last_in)(cross_in(False).start)

    lax.fori_loop(0, n_rows, send_up, 0)

    def mix(out, lo, hi, rows):
        out[rows, :] = third(lo[rows, :], out[rows, :], hi[rows, :])

    def mix_gate(i, carry):
        for copy in g_copies(i):
            copy.wait()
        mix(og, glo, ghi, rest(i))
        return carry

    lax.fori_loop(0, n_rest, mix_gate, 0)
    lax.fori_loop(0, 1, mix_down, 0)
    ahead, behind = b_copies()
    pl.when(lower)(ahead.wait_send)
    pl.when(upper)(behind.wait_send)

    @pl.when(inside)
    def _():
        cross_in(True).wait_recv()
        both = summing[...].astype(F32) + og[rows_b, :].astype(F32)
        summing[...] = both.astype(BF16)
        pl.when(first_in)(cross_end(True).start)
        pl.when(last_in)(cross_end(False).start)
        cross_out(True).wait_send()
        mix(og, glo, ghi, rows_b)

    def mix_up(i, carry):
        for copy in u_copies(i):
            copy.wait()
        mix(ou, ulo, uhi, cols(i, ROWS))
        return carry

    lax.fori_loop(0, n_rows, mix_up, 0)

    def end(own, both):
        return ((own.astype(F32) + both.astype(F32)) / 3.0).astype(BF16)

    relay_over().wait_send()

    @pl.when(inside)
    def _():
        cross_in(True).wait_send()
        cross_end(True).wait_send()

    @pl.when(first_end)
    def _():
        cross_end(True).wait_recv()
        og[rows_b, :] = end(og[rows_b, :], ghi[rows_b, :])

    @pl.when(last_end)
    def _():
        cross_end(False).wait_recv()
        og[rows_b, :] = end(og[rows_b, :], glo[rows_b, :])


def write_kernel(pieces, *refs):
    held, out, sem = refs[:3], refs[3:6], refs[6]
    copies = []
    for i in range(3):
        rows = held[i].shape[0] // pieces
        for p in range(pieces):
            part = pl.ds(p * rows, rows)
            copies.append(
                pltpu.make_async_copy(held[i].at[part, :], out[i].at[0, part, :], sem.at[i, p])
            )
    for copy in copies:
        copy.start()
    for copy in copies:
        copy.wait()


def write_out(*arrays):
    pieces = 4
    return pl.pallas_call(
        functools.partial(write_kernel, pieces),
        out_shape=tuple(jax.ShapeDtypeStruct((1, *a.shape), a.dtype) for a in arrays),
        in_specs=[pl.BlockSpec(memory_space=pltpu.VMEM)] * 3,
        out_specs=(pl.BlockSpec(memory_space=pl.ANY),) * 3,
        scratch_shapes=[pltpu.SemaphoreType.DMA((3, pieces))],
        compiler_params=pltpu.CompilerParams(vmem_limit_bytes=16 * 2**20),
    )(*arrays)


def local(replicas, tokens, targets, gate_weight, up_weight, down_weight):
    toks, width = tokens.shape[1:]
    units = gate_weight.shape[2]
    n_cols, n_rows, n_units = width // COLS, width // ROWS, units // COLS
    n_rest = (width - AWAY) // REST
    half = toks // 2
    dma = pltpu.SemaphoreType.DMA
    any_spec = pl.BlockSpec(memory_space=pl.ANY)
    vmem_spec = pl.BlockSpec(memory_space=pltpu.VMEM)
    received = jax.ShapeDtypeStruct((n_cols, units, COLS), BF16)
    gate_out, up_out, down_out, *_ = pl.pallas_call(
        functools.partial(kernel, replicas),
        out_shape=(
            pltpu.VMEM((width, units), BF16),
            pltpu.VMEM((width, units), BF16),
            pltpu.VMEM((units, width), BF16),
            received,
            received,
            jax.ShapeDtypeStruct((FIRST, COLS), BF16),
        ),
        in_specs=[any_spec] * 5,
        out_specs=(vmem_spec, vmem_spec, vmem_spec, any_spec, any_spec, any_spec),
        scratch_shapes=[
            pltpu.VMEM((toks, width), BF16),
            pltpu.VMEM((half, width), BF16),
            pltpu.VMEM((toks, 1), F32),
            pltpu.VMEM((toks, width), BF16),
            pltpu.VMEM((units, width), BF16),
            pltpu.VMEM((toks, units), F32),
            pltpu.VMEM((toks, units), F32),
            pltpu.VMEM((toks, units), BF16),
            pltpu.VMEM((units, toks), BF16),
            pltpu.VMEM((toks, width), BF16),
            pltpu.VMEM((toks, units), BF16),
            pltpu.VMEM((toks, units), BF16),
            pltpu.VMEM((toks, width), BF16),
            pltpu.VMEM((half, width), BF16),
            pltpu.VMEM((half, width), BF16),
            pltpu.VMEM((width, units), BF16),
            pltpu.VMEM((width, units), BF16),
            pltpu.VMEM((width, units), BF16),
            pltpu.VMEM((width, units), BF16),
            pltpu.VMEM((2, units, COLS), BF16),
            pltpu.VMEM((AWAY, units), BF16),
            pltpu.VMEM((AWAY, units), BF16),
            dma((4,)),
            dma((2,)),
            dma((2, n_units)),
            dma((n_cols + COLS // HEAD - 1,)),
            dma((n_cols + COLS // HEAD - 1,)),
            dma((n_cols + COLS // HEAD - 1,)),
            dma((n_cols + COLS // HEAD - 1,)),
            dma((n_cols + COLS // HEAD - 1,)),
            dma((n_cols + COLS // HEAD - 1,)),
            dma((2, n_cols)),
            dma((2, n_cols)),
            dma((2, n_rest)),
            dma((2, n_rest)),
            dma((2, n_rows)),
            dma((2, n_rows)),
            dma((2,)),
            dma((2,)),
            dma((2,)),
            dma((3,)),
            dma((6,)),
            pltpu.SemaphoreType.REGULAR,
        ],
        compiler_params=pltpu.CompilerParams(
            collective_id=0, has_side_effects=True, vmem_limit_bytes=50 * 2**20
        ),
    )(tokens[0], targets[0], gate_weight[0], up_weight[0], down_weight[0])
    return write_out(gate_out, up_out, down_out)


def solution(mesh):
    placed = (
        P("gossip", None, None),
        P("gossip", None, None),
        P("gossip", None, "mp"),
        P("gossip", None, "mp"),
        P("gossip", "mp", None),
    )
    return jax.shard_map(
        functools.partial(local, mesh.shape["gossip"]),
        mesh=mesh,
        in_specs=placed,
        out_specs=(P("gossip", None, "mp"), P("gossip", None, "mp"), P("gossip", "mp", None)),
        check_vma=False,
    )
```

```python
import functools

import jax
import jax.numpy as jnp
from jax import lax
from jax.experimental import pallas as pl
from jax.experimental.pallas import tpu as pltpu
from jax.sharding import PartitionSpec as P

MESH = pl.DeviceIdType.MESH
F32 = jnp.float32
BF16 = jnp.bfloat16
COLS = 256
X, Y = 4, 2
ROWS = 256
REST = 272
AWAY = 144
FIRST = 512
DETOUR = 2
HEAD = 128


def dot(a, b, dims):
    return lax.dot_general(a, b, (dims, ((), ())), preferred_element_type=F32)


def kernel(
    replicas,
    tok_h, tgt_h, wg_h, wu_h, wd_h,
    og, ou, od, lo_h, hi_h,
    x, tg, inv, nrm, wd, slope, act, hid, hid_t, err, gg, gu,
    part, part_in, sum_in, passing, glo, ghi, ulo, uhi, stage, crossing, summing, relayed,
    tok_sem, load_sem, w_sem, p_send, p_recv, q_send, q_recv, e_send, e_recv,
    d_send, d_recv, g_send, g_recv, u_send, u_recv, st_sem,
    b_send, b_recv, relay_sem, cross_sem, pass_sem, go_sem,
):
    g = lax.axis_index("gossip")
    m = lax.axis_index("mp")
    core = lax.rem(m, 2)
    sibling = m + 1 - 2 * core
    peer = lax.rem(m + 2, 4)
    after = lax.rem(g + 1, replicas)
    before = lax.rem(g + replicas - 1, replicas)
    toks, width = x.shape
    units = wd.shape[0]
    half = toks // 2
    in_scale = 1.0 / width**0.5
    mid_scale = 1.0 / (4 * units) ** 0.5
    step_size = (4 * units) / 4.0

    def cols(i, size=COLS):
        return pl.ds(pl.multiple_of(i * size, size), size)

    n_cols = width // COLS
    n_rows = width // ROWS
    n_rest = (width - AWAY) // REST
    rows_b = pl.ds(0, AWAY)
    early, late = pl.ds(0, FIRST), pl.ds(FIRST, units - FIRST)
    n_units = units // COLS
    mine = pl.ds(pl.multiple_of(core * half, half), half)
    theirs = pl.ds(pl.multiple_of((1 - core) * half, half), half)

    piece = toks // 4

    def tok_copy(i):
        rows = cols(i, piece)
        return pltpu.make_async_copy(tok_h.at[rows, :], x.at[rows, :], tok_sem.at[i])

    for i in range(4):
        tok_copy(i).start()

    def w_copies(f):
        return (
            pltpu.make_async_copy(wg_h.at[:, cols(f)], og.at[:, cols(f)], w_sem.at[0, f]),
            pltpu.make_async_copy(wu_h.at[:, cols(f)], ou.at[:, cols(f)], w_sem.at[1, f]),
        )

    for copy in w_copies(0):
        copy.start()

    wd_copy = pltpu.make_async_copy(wd_h, wd, load_sem.at[0])
    tgt_copy = pltpu.make_async_copy(tgt_h.at[mine, :], tg, load_sem.at[1])

    along = lax.rem(g, X)
    last_end = along == X - 1
    first_end = along == 0
    at_end = jnp.logical_or(last_end, first_end)
    layer = g // (X * Y)
    layers = replicas // (X * Y)
    beyond = lax.rem(layer + (along // (X - 1)) * 2 - 1 + layers, layers)
    facing = [
        (at * (X * Y) + row * X + (X - 1 - along), shard)
        for at in (layer, beyond)
        for row in range(Y)
        for shard in range(4)
    ]

    def tell(sem, wheres):
        for where in wheres:
            pl.semaphore_signal(sem, inc=1, device_id=where, device_id_type=MESH)

    barrier = pltpu.get_barrier_semaphore()
    far_end = g + (X - 1) * (1 - 2 * (along // (X - 1)))
    diagonal = lax.rem(g + (X + 1) * (1 - 2 * lax.rem(along, 2)) + replicas, replicas)
    across_up = lax.rem(g + X, replicas)
    across_down = lax.rem(g - X + replicas, replicas)
    beside = g + 1 - 2 * lax.rem(along, 2)
    near = ((g, sibling), (g, peer), (diagonal, m), (beside, peer))
    inward = g + 1 - 2 * (along // (X - 1))

    @pl.when(jnp.logical_not(at_end))
    def _():
        tell(barrier, (*near, (after, m), (before, m), (across_up, m), (across_down, m)))

    @pl.when(at_end)
    def _():
        tell(barrier, (*near, (inward, m), *facing))

    def square(i, carry):
        rows = cols(i, 64)
        wide = x[rows, :].astype(F32)
        mean = jnp.mean(wide * wide, axis=-1, keepdims=True)
        inv[rows, :] = lax.rsqrt(mean + 1e-06)
        return carry

    for i in range(4):
        tok_copy(i).wait()
        lax.fori_loop(i * piece // 64, (i + 1) * piece // 64, square, 0)
        for copy in w_copies(i + 1) if i + 1 < n_units else (wd_copy, tgt_copy):
            copy.start()

    def forward(f, carry):
        for copy in w_copies(f):
            copy.wait()
        scale = inv[...] * in_scale
        gate = dot(x[...], og[:, cols(f)], ((1,), (0,))) * scale
        up = dot(x[...], ou[:, cols(f)], ((1,), (0,))) * scale
        sig = jax.nn.sigmoid(gate)
        acted = gate * sig
        act[:, cols(f)] = acted
        slope[:, cols(f)] = up * (sig * (1.0 + gate * (1.0 - sig)))
        hid[:, cols(f)] = (acted * up).astype(BF16)
        return carry

    lax.fori_loop(0, n_units, forward, 0)
    wd_copy.wait()

    @pl.when(jnp.logical_not(at_end))
    def _():
        pl.semaphore_wait(barrier, len(near) + 4)

    @pl.when(at_end)
    def _():
        pl.semaphore_wait(barrier, len(near) + 1 + len(facing))

    def head(i):
        return cols(i, HEAD), i

    def block(d):
        return cols(d), d + COLS // HEAD - 1

    n_heads = COLS // HEAD
    last = n_cols + n_heads - 2 - DETOUR
    inside = jnp.logical_not(at_end)

    def p_copy(at, k):
        return pltpu.make_async_remote_copy(
            src_ref=part.at[theirs, at], dst_ref=part_in.at[:, at],
            send_sem=p_send.at[k], recv_sem=p_recv.at[k],
            device_id=(g, sibling), device_id_type=MESH,
        )

    def q_copy(at, k):
        return pltpu.make_async_remote_copy(
            src_ref=part.at[mine, at], dst_ref=sum_in.at[:, at],
            send_sem=q_send.at[k], recv_sem=q_recv.at[k],
            device_id=(g, peer), device_id_type=MESH,
        )

    def detour_out(i):
        d = n_cols - DETOUR + i
        return pltpu.make_async_remote_copy(
            src_ref=part.at[mine, cols(d)], dst_ref=passing.at[i],
            send_sem=q_send.at[block(d)[1]], recv_sem=pass_sem.at[0, i],
            device_id=(beside, peer), device_id_type=MESH,
        )

    def detour_on(i):
        d = n_cols - DETOUR + i
        return pltpu.make_async_remote_copy(
            src_ref=passing.at[i], dst_ref=sum_in.at[:, cols(d)],
            send_sem=pass_sem.at[1, i], recv_sem=q_recv.at[block(d)[1]],
            device_id=(beside, m), device_id_type=MESH,
        )

    def e_copy(at, k):
        return pltpu.make_async_remote_copy(
            src_ref=err.at[mine, at], dst_ref=err.at[mine, at],
            send_sem=e_send.at[k], recv_sem=e_recv.at[k],
            device_id=(g, sibling), device_id_type=MESH,
        )

    def pair(src, lo, hi, send, recv, i):
        def sem(sems, k):
            return sems.at[k] if i is None else sems.at[k, i]

        return (
            pltpu.make_async_remote_copy(
                src_ref=src, dst_ref=lo, send_sem=sem(send, 0), recv_sem=sem(recv, 0),
                device_id=(after, m), device_id_type=MESH,
            ),
            pltpu.make_async_remote_copy(
                src_ref=src, dst_ref=hi, send_sem=sem(send, 1), recv_sem=sem(recv, 1),
                device_id=(before, m), device_id_type=MESH,
            ),
        )

    def d_copies(d):
        return pair(od.at[:, cols(d)], lo_h.at[d], hi_h.at[d], d_send, d_recv, d)

    def g_pair(rows, send, recv, i):
        return pair(og.at[rows, :], glo.at[rows, :], ghi.at[rows, :], send, recv, i)

    def rest(i):
        return pl.ds(pl.multiple_of(AWAY + i * REST, 16), REST)

    def g_copies(i):
        return g_pair(rest(i), g_send, g_recv, i)

    def b_copies():
        return g_pair(rows_b, b_send, b_recv, None)

    def u_copies(i):
        rows = cols(i, ROWS)
        return pair(ou.at[rows, :], ulo.at[rows, :], uhi.at[rows, :], u_send, u_recv, i)

    def send(src, dst, send_sem, recv_sem, replica):
        return pltpu.make_async_remote_copy(
            src_ref=src, dst_ref=dst, send_sem=send_sem, recv_sem=recv_sem,
            device_id=(replica, m), device_id_type=MESH,
        )

    def relay_out():
        return send(od.at[early, cols(1)], relayed, relay_sem.at[0], relay_sem.at[1], far_end)

    def relay_over():
        return send(relayed, relayed, relay_sem.at[2], relay_sem.at[1], diagonal)

    def relay_on(first):
        dst, k, where = (lo_h, 0, before) if first else (hi_h, 1, after)
        return send(relayed, dst.at[1, early, :], relay_sem.at[2], d_recv.at[k, 1], where)

    def late_copies():
        return (
            send(od.at[late, cols(1)], lo_h.at[1, late, :], d_send.at[0, 1], d_recv.at[0, 1], after),
            send(od.at[late, cols(1)], hi_h.at[1, late, :], d_send.at[1, 1], d_recv.at[1, 1], before),
        )

    def cross_out(first):
        src, where = (glo, across_down) if first else (ghi, across_up)
        return send(src.at[rows_b, :], crossing, cross_sem.at[0], cross_sem.at[1], where)

    def cross_in(first):
        return send(crossing, summing, cross_sem.at[2], cross_sem.at[3], after if first else before)

    def cross_end(first):
        dst, where = (ghi, before) if first else (glo, after)
        return send(summing, dst.at[rows_b, :], cross_sem.at[4], cross_sem.at[5], where)

    def partial(d, carry):
        part[:, cols(d)] = dot(hid[...], wd[:, cols(d)], ((1,), (0,))).astype(BF16)

        @pl.when(d == 0)
        def _():
            for i in range(n_heads):
                p_copy(*head(i)).start()

        pl.when(d > 0)(p_copy(*block(d)).start)
        return carry

    def join(at, k):
        p_copy(at, k).wait()
        total = part[mine, at].astype(F32) + part_in[:, at].astype(F32)
        part[mine, at] = total.astype(BF16)
        straight = jnp.logical_or(k <= last, inside)
        pl.when(straight)(q_copy(at, k).start)
        pl.when(jnp.logical_not(straight))(detour_out(jnp.maximum(k - last - 1, 0)).start)

    def join_head(i, carry):
        join(*head(i))
        return carry

    def spread(d, carry):
        partial(d, carry)
        join(*block(d - 1))
        return carry

    lax.fori_loop(0, 2, partial, 0)
    lax.fori_loop(0, n_heads, join_head, 0)
    lax.fori_loop(2, n_cols, spread, 0)
    join(*block(n_cols - 1))

    def turn(i, carry):
        hid_t[cols(i), :] = hid[:, cols(i)].T
        return carry

    lax.fori_loop(0, n_units, turn, 0)

    def norm(i, carry):
        rows = cols(i, 64)
        nrm[rows, :] = (x[rows, :].astype(F32) * inv[rows, :]).astype(BF16)
        return carry

    tgt_copy.wait()

    def step_down(at, k):
        q_copy(at, k).wait()

        @pl.when(jnp.logical_and(at_end, k == last))
        def _():
            tell(go_sem, facing)

        total = part[mine, at].astype(F32) + sum_in[:, at].astype(F32)
        offset = x[mine, at].astype(F32) - tg[:, at].astype(F32)
        err[mine, at] = ((offset + total * mid_scale) / toks).astype(BF16)
        e_copy(at, k).start()
        e_copy(at, k).wait()
        grad = dot(hid_t[...], err[:, at], ((1,), (0,)))
        od[:, at] = (wd[:, at].astype(F32) - (step_size * mid_scale) * grad).astype(BF16)

    def inward_start(ahead, behind):
        pl.when(jnp.logical_not(last_end))(ahead.start)
        pl.when(jnp.logical_not(first_end))(behind.start)

    def down_head(i, carry):
        at, k = head(i)
        step_down(at, k)
        inward_start(
            *pair(od.at[:, at], lo_h.at[0, :, at], hi_h.at[0, :, at], d_send, d_recv, 0)
        )
        return carry

    def down(d, carry):
        @pl.when(jnp.logical_and(inside, d <= DETOUR))
        def _():
            i = jnp.minimum(d, DETOUR) - 1
            detour_out(i).wait_recv()
            detour_on(i).start()

        step_down(*block(d))

        @pl.when(d != 1)
        def _():
            inward_start(*d_copies(d))

        @pl.when(d == 1)
        def _():
            ahead, behind = d_copies(1)
            late_ahead, late_behind = late_copies()
            pl.when(along <= 1)(ahead.start)
            pl.when(along >= 2)(behind.start)
            pl.when(along == 2)(late_ahead.start)
            pl.when(along == 1)(late_behind.start)
            pl.when(at_end)(relay_out().start)

        return carry

    def down_late(d, carry):
        step_down(*block(d))
        for copy in d_copies(d):
            copy.start()
        return carry

    lax.fori_loop(0, n_heads, down_head, 0)
    lax.fori_loop(0, toks // 64, norm, 0)
    lax.fori_loop(1, n_cols - DETOUR, down, 0)

    @pl.when(at_end)
    def _():
        pl.semaphore_wait(go_sem, len(facing))

    def held_back(d, carry):
        ahead, behind = d_copies(d)
        pl.when(last_end)(ahead.start)
        pl.when(first_end)(behind.start)
        return carry

    held_back(0, 0)
    ahead, behind = late_copies()
    pl.when(last_end)(ahead.start)
    pl.when(first_end)(behind.start)
    lax.fori_loop(2, n_cols - DETOUR, held_back, 0)
    lax.fori_loop(n_cols - DETOUR, n_cols, down_late, 0)

    def back(f, carry):
        grad = dot(err[...], wd[cols(f), :], ((1,), (1,))) * mid_scale
        gg[:, cols(f)] = (grad * slope[:, cols(f)]).astype(BF16)
        gu[:, cols(f)] = (grad * act[:, cols(f)]).astype(BF16)
        return carry

    lax.fori_loop(0, n_units, back, 0)

    @pl.when(at_end)
    def _():
        relay_out().wait_recv()
        relay_over().start()

    def step(out, grads, rows):
        grad = dot(nrm[:, rows], grads[...], ((0,), (0,)))
        out[rows, :] = (out[rows, :].astype(F32) - (step_size * in_scale) * grad).astype(BF16)

    def step_up(i, carry):
        step(ou, gu, cols(i, ROWS))
        return carry

    def send_up(i, carry):
        for copy in u_copies(i):
            copy.start()
        return carry

    lower, upper = along <= 1, along >= 2
    first_in, last_in = along == 1, along == 2

    def step_gate(i, carry):
        step(og, gg, pl.ds(pl.multiple_of(i * 128, 128), 128))
        return carry

    def send_gate(i, carry):
        for copy in g_copies(i):
            copy.start()
        return carry

    lax.fori_loop(0, width // 128, step_gate, 0)
    ahead, behind = b_copies()
    pl.when(lower)(ahead.start)
    pl.when(upper)(behind.start)
    lax.fori_loop(0, n_rest, send_gate, 0)
    lax.fori_loop(0, n_rows, step_up, 0)

    def third(lo, own, hi):
        return ((lo.astype(F32) + own.astype(F32) + hi.astype(F32)) / 3.0).astype(BF16)

    def mix_down(d, carry):
        for copy in d_copies(d):
            copy.wait()
        loads = [
            pltpu.make_async_copy(lo_h.at[d], stage.at[0], st_sem.at[0]),
            pltpu.make_async_copy(hi_h.at[d], stage.at[1], st_sem.at[1]),
        ]
        for load in loads:
            load.start()
        for load in loads:
            load.wait()
        od[:, cols(d)] = third(stage[0], od[:, cols(d)], stage[1])
        return carry

    mix_down(0, 0)
    lax.fori_loop(2, n_cols, mix_down, 0)

    @pl.when(inside)
    def _():
        relay_out().wait_recv()
        both = relayed[...].astype(F32) + od[early, cols(1)].astype(F32)
        relayed[...] = both.astype(BF16)
        pl.when(first_in)(relay_on(True).start)
        pl.when(last_in)(relay_on(False).start)
        for copy in b_copies():
            copy.wait_recv()
        pl.when(first_in)(cross_out(True).start)
        pl.when(last_in)(cross_out(False).start)
        cross_out(True).wait_recv()
        pl.when(first_in)(cross_in(True).start)
        pl.when(last_in)(cross_in(False).start)

    lax.fori_loop(0, n_rows, send_up, 0)

    def mix(out, lo, hi, rows):
        out[rows, :] = third(lo[rows, :], out[rows, :], hi[rows, :])

    def mix_gate(i, carry):
        for copy in g_copies(i):
            copy.wait()
        mix(og, glo, ghi, rest(i))
        return carry

    lax.fori_loop(0, n_rest, mix_gate, 0)
    ahead, behind = d_copies(1)
    late_ahead, late_behind = late_copies()
    pl.when(lower)(ahead.wait_send)
    pl.when(upper)(behind.wait_send)
    pl.when(upper)(late_ahead.wait_send)
    pl.when(lower)(late_behind.wait_send)
    pl.when(at_end)(relay_out().wait_send)
    pl.when(jnp.logical_not(last_end))(ahead.wait_recv)
    pl.when(jnp.logical_not(first_end))(behind.wait_recv)
    pl.when(last_end)(late_ahead.wait_recv)
    pl.when(first_end)(late_behind.wait_recv)

    def load_second(rows, k):
        held = hi_h if k else lo_h
        return pltpu.make_async_copy(held.at[1, rows, :], stage.at[k, rows, :], st_sem.at[k])

    def third_second(rows):
        loads = [load_second(rows, k) for k in range(2)]
        for load in loads:
            load.start()
        for load in loads:
            load.wait()
        od[rows, cols(1)] = third(stage[0, rows, :], od[rows, cols(1)], stage[1, rows, :])

    third_second(late)

    @pl.when(inside)
    def _():
        third_second(early)

    def end(own, both):
        return ((own.astype(F32) + both.astype(F32)) / 3.0).astype(BF16)

    def end_second(k):
        load = load_second(early, k)
        load.start()
        load.wait()
        od[early, cols(1)] = end(od[early, cols(1)], stage[k, early, :])

    @pl.when(first_end)
    def _():
        end_second(0)

    @pl.when(last_end)
    def _():
        end_second(1)

    ahead, behind = b_copies()
    pl.when(lower)(ahead.wait_send)
    pl.when(upper)(behind.wait_send)

    @pl.when(inside)
    def _():
        cross_in(True).wait_recv()
        both = summing[...].astype(F32) + og[rows_b, :].astype(F32)
        summing[...] = both.astype(BF16)
        pl.when(first_in)(cross_end(True).start)
        pl.when(last_in)(cross_end(False).start)
        cross_out(True).wait_send()
        mix(og, glo, ghi, rows_b)

    def mix_up(i, carry):
        for copy in u_copies(i):
            copy.wait()
        mix(ou, ulo, uhi, cols(i, ROWS))
        return carry

    lax.fori_loop(0, n_rows, mix_up, 0)

    relay_over().wait_send()

    @pl.when(inside)
    def _():
        for i in range(DETOUR):
            detour_on(i).wait_send()

    @pl.when(inside)
    def _():
        cross_in(True).wait_send()
        cross_end(True).wait_send()

    @pl.when(first_end)
    def _():
        cross_end(True).wait_recv()
        og[rows_b, :] = end(og[rows_b, :], ghi[rows_b, :])

    @pl.when(last_end)
    def _():
        cross_end(False).wait_recv()
        og[rows_b, :] = end(og[rows_b, :], glo[rows_b, :])


def write_kernel(pieces, *refs):
    held, out, sem = refs[:3], refs[3:6], refs[6]
    copies = []
    for i in range(3):
        rows = held[i].shape[0] // pieces
        for p in range(pieces):
            part = pl.ds(p * rows, rows)
            copies.append(
                pltpu.make_async_copy(held[i].at[part, :], out[i].at[0, part, :], sem.at[i, p])
            )
    for copy in copies:
        copy.start()
    for copy in copies:
        copy.wait()


def write_out(*arrays):
    pieces = 4
    return pl.pallas_call(
        functools.partial(write_kernel, pieces),
        out_shape=tuple(jax.ShapeDtypeStruct((1, *a.shape), a.dtype) for a in arrays),
        in_specs=[pl.BlockSpec(memory_space=pltpu.VMEM)] * 3,
        out_specs=(pl.BlockSpec(memory_space=pl.ANY),) * 3,
        scratch_shapes=[pltpu.SemaphoreType.DMA((3, pieces))],
        compiler_params=pltpu.CompilerParams(vmem_limit_bytes=16 * 2**20),
    )(*arrays)


def local(replicas, tokens, targets, gate_weight, up_weight, down_weight):
    toks, width = tokens.shape[1:]
    units = gate_weight.shape[2]
    n_cols, n_rows, n_units = width // COLS, width // ROWS, units // COLS
    n_rest = (width - AWAY) // REST
    half = toks // 2
    dma = pltpu.SemaphoreType.DMA
    any_spec = pl.BlockSpec(memory_space=pl.ANY)
    vmem_spec = pl.BlockSpec(memory_space=pltpu.VMEM)
    received = jax.ShapeDtypeStruct((n_cols, units, COLS), BF16)
    gate_out, up_out, down_out, *_ = pl.pallas_call(
        functools.partial(kernel, replicas),
        out_shape=(
            pltpu.VMEM((width, units), BF16),
            pltpu.VMEM((width, units), BF16),
            pltpu.VMEM((units, width), BF16),
            received,
            received,
        ),
        in_specs=[any_spec] * 5,
        out_specs=(vmem_spec, vmem_spec, vmem_spec, any_spec, any_spec),
        scratch_shapes=[
            pltpu.VMEM((toks, width), BF16),
            pltpu.VMEM((half, width), BF16),
            pltpu.VMEM((toks, 1), F32),
            pltpu.VMEM((toks, width), BF16),
            pltpu.VMEM((units, width), BF16),
            pltpu.VMEM((toks, units), F32),
            pltpu.VMEM((toks, units), F32),
            pltpu.VMEM((toks, units), BF16),
            pltpu.VMEM((units, toks), BF16),
            pltpu.VMEM((toks, width), BF16),
            pltpu.VMEM((toks, units), BF16),
            pltpu.VMEM((toks, units), BF16),
            pltpu.VMEM((toks, width), BF16),
            pltpu.VMEM((half, width), BF16),
            pltpu.VMEM((half, width), BF16),
            pltpu.VMEM((DETOUR, half, COLS), BF16),
            pltpu.VMEM((width, units), BF16),
            pltpu.VMEM((width, units), BF16),
            pltpu.VMEM((width, units), BF16),
            pltpu.VMEM((width, units), BF16),
            pltpu.VMEM((2, units, COLS), BF16),
            pltpu.VMEM((AWAY, units), BF16),
            pltpu.VMEM((AWAY, units), BF16),
            pltpu.VMEM((FIRST, COLS), BF16),
            dma((4,)),
            dma((2,)),
            dma((2, n_units)),
            dma((n_cols + COLS // HEAD - 1,)),
            dma((n_cols + COLS // HEAD - 1,)),
            dma((n_cols + COLS // HEAD - 1,)),
            dma((n_cols + COLS // HEAD - 1,)),
            dma((n_cols + COLS // HEAD - 1,)),
            dma((n_cols + COLS // HEAD - 1,)),
            dma((2, n_cols)),
            dma((2, n_cols)),
            dma((2, n_rest)),
            dma((2, n_rest)),
            dma((2, n_rows)),
            dma((2, n_rows)),
            dma((2,)),
            dma((2,)),
            dma((2,)),
            dma((3,)),
            dma((6,)),
            dma((2, DETOUR)),
            pltpu.SemaphoreType.REGULAR,
        ],
        compiler_params=pltpu.CompilerParams(
            collective_id=0, has_side_effects=True, vmem_limit_bytes=50 * 2**20
        ),
    )(tokens[0], targets[0], gate_weight[0], up_weight[0], down_weight[0])
    return write_out(gate_out, up_out, down_out)


def solution(mesh):
    placed = (
        P("gossip", None, None),
        P("gossip", None, None),
        P("gossip", None, "mp"),
        P("gossip", None, "mp"),
        P("gossip", "mp", None),
    )
    return jax.shard_map(
        functools.partial(local, mesh.shape["gossip"]),
        mesh=mesh,
        in_specs=placed,
        out_specs=(P("gossip", None, "mp"), P("gossip", None, "mp"), P("gossip", "mp", None)),
        check_vma=False,
    )
```

```python
import functools

import jax
import jax.numpy as jnp
from jax import lax
from jax.experimental import pallas as pl
from jax.experimental.pallas import tpu as pltpu
from jax.sharding import PartitionSpec as P

MESH = pl.DeviceIdType.MESH
F32 = jnp.float32
BF16 = jnp.bfloat16
COLS = 256
X, Y = 4, 2
ROWS = 256
REST = 208
AWAY = 176
FIRST = 448
DETOUR = 2
HEAD = 128


def dot(a, b, dims):
    return lax.dot_general(a, b, (dims, ((), ())), preferred_element_type=F32)


def kernel(
    replicas,
    tok_h, tgt_h, wg_h, wu_h, wd_h,
    og, ou, od, lo_h, hi_h,
    x, tg, inv, nrm, wd, slope, act, hid, hid_t, err, gg, gu,
    part, part_in, sum_in, passing, glo, ghi, ulo, uhi, stage, crossing, summing, relayed,
    tok_sem, load_sem, w_sem, p_send, p_recv, q_send, q_recv, e_send, e_recv,
    d_send, d_recv, g_send, g_recv, u_send, u_recv, st_sem,
    b_send, b_recv, relay_sem, cross_sem, pass_sem, go_sem,
):
    g = lax.axis_index("gossip")
    m = lax.axis_index("mp")
    core = lax.rem(m, 2)
    sibling = m + 1 - 2 * core
    peer = lax.rem(m + 2, 4)
    after = lax.rem(g + 1, replicas)
    before = lax.rem(g + replicas - 1, replicas)
    toks, width = x.shape
    units = wd.shape[0]
    half = toks // 2
    in_scale = 1.0 / width**0.5
    mid_scale = 1.0 / (4 * units) ** 0.5
    step_size = (4 * units) / 4.0

    def cols(i, size=COLS):
        return pl.ds(pl.multiple_of(i * size, size), size)

    n_cols = width // COLS
    n_rows = width // ROWS
    n_rest = (width - AWAY) // REST
    rows_b = pl.ds(0, AWAY)
    early, late = pl.ds(0, FIRST), pl.ds(FIRST, units - FIRST)
    n_units = units // COLS
    mine = pl.ds(pl.multiple_of(core * half, half), half)
    theirs = pl.ds(pl.multiple_of((1 - core) * half, half), half)

    piece = toks // 4

    def tok_copy(i):
        rows = cols(i, piece)
        return pltpu.make_async_copy(tok_h.at[rows, :], x.at[rows, :], tok_sem.at[i])

    for i in range(4):
        tok_copy(i).start()

    def w_copies(f):
        return (
            pltpu.make_async_copy(wg_h.at[:, cols(f)], og.at[:, cols(f)], w_sem.at[0, f]),
            pltpu.make_async_copy(wu_h.at[:, cols(f)], ou.at[:, cols(f)], w_sem.at[1, f]),
        )

    for copy in w_copies(0):
        copy.start()

    wd_copy = pltpu.make_async_copy(wd_h, wd, load_sem.at[0])
    tgt_copy = pltpu.make_async_copy(tgt_h.at[mine, :], tg, load_sem.at[1])

    along = lax.rem(g, X)
    last_end = along == X - 1
    first_end = along == 0
    at_end = jnp.logical_or(last_end, first_end)
    layer = g // (X * Y)
    layers = replicas // (X * Y)
    beyond = lax.rem(layer + (along // (X - 1)) * 2 - 1 + layers, layers)
    facing = [
        (at * (X * Y) + row * X + (X - 1 - along), shard)
        for at in (layer, beyond)
        for row in range(Y)
        for shard in range(4)
    ]

    def tell(sem, wheres):
        for where in wheres:
            pl.semaphore_signal(sem, inc=1, device_id=where, device_id_type=MESH)

    barrier = pltpu.get_barrier_semaphore()
    far_end = g + (X - 1) * (1 - 2 * (along // (X - 1)))
    diagonal = lax.rem(g + (X + 1) * (1 - 2 * lax.rem(along, 2)) + replicas, replicas)
    across_up = lax.rem(g + X, replicas)
    across_down = lax.rem(g - X + replicas, replicas)
    beside = g + 1 - 2 * lax.rem(along, 2)
    near = ((g, sibling), (g, peer), (diagonal, m), (beside, peer))
    inward = g + 1 - 2 * (along // (X - 1))

    @pl.when(jnp.logical_not(at_end))
    def _():
        tell(barrier, (*near, (after, m), (before, m), (across_up, m), (across_down, m)))

    @pl.when(at_end)
    def _():
        tell(barrier, (*near, (inward, m), *facing))

    def square(i, carry):
        rows = cols(i, 64)
        wide = x[rows, :].astype(F32)
        mean = jnp.mean(wide * wide, axis=-1, keepdims=True)
        inv[rows, :] = lax.rsqrt(mean + 1e-06)
        return carry

    for i in range(4):
        tok_copy(i).wait()
        lax.fori_loop(i * piece // 64, (i + 1) * piece // 64, square, 0)
        for copy in w_copies(i + 1) if i + 1 < n_units else (wd_copy, tgt_copy):
            copy.start()

    def forward(f, carry):
        for copy in w_copies(f):
            copy.wait()
        scale = inv[...] * in_scale
        gate = dot(x[...], og[:, cols(f)], ((1,), (0,))) * scale
        up = dot(x[...], ou[:, cols(f)], ((1,), (0,))) * scale
        sig = jax.nn.sigmoid(gate)
        acted = gate * sig
        act[:, cols(f)] = acted
        slope[:, cols(f)] = up * (sig * (1.0 + gate * (1.0 - sig)))
        hid[:, cols(f)] = (acted * up).astype(BF16)
        return carry

    lax.fori_loop(0, n_units, forward, 0)
    wd_copy.wait()

    @pl.when(jnp.logical_not(at_end))
    def _():
        pl.semaphore_wait(barrier, len(near) + 4)

    @pl.when(at_end)
    def _():
        pl.semaphore_wait(barrier, len(near) + 1 + len(facing))

    def head(i):
        return cols(i, HEAD), i

    def block(d):
        return cols(d), d + COLS // HEAD - 1

    n_heads = COLS // HEAD
    last = n_cols + n_heads - 2 - DETOUR
    inside = jnp.logical_not(at_end)

    def p_copy(at, k):
        return pltpu.make_async_remote_copy(
            src_ref=part.at[theirs, at], dst_ref=part_in.at[:, at],
            send_sem=p_send.at[k], recv_sem=p_recv.at[k],
            device_id=(g, sibling), device_id_type=MESH,
        )

    def q_copy(at, k):
        return pltpu.make_async_remote_copy(
            src_ref=part.at[mine, at], dst_ref=sum_in.at[:, at],
            send_sem=q_send.at[k], recv_sem=q_recv.at[k],
            device_id=(g, peer), device_id_type=MESH,
        )

    def detour_out(i):
        d = n_cols - DETOUR + i
        return pltpu.make_async_remote_copy(
            src_ref=part.at[mine, cols(d)], dst_ref=passing.at[i],
            send_sem=q_send.at[block(d)[1]], recv_sem=pass_sem.at[0, i],
            device_id=(beside, peer), device_id_type=MESH,
        )

    def detour_on(i):
        d = n_cols - DETOUR + i
        return pltpu.make_async_remote_copy(
            src_ref=passing.at[i], dst_ref=sum_in.at[:, cols(d)],
            send_sem=pass_sem.at[1, i], recv_sem=q_recv.at[block(d)[1]],
            device_id=(beside, m), device_id_type=MESH,
        )

    def e_copy(at, k):
        return pltpu.make_async_remote_copy(
            src_ref=err.at[mine, at], dst_ref=err.at[mine, at],
            send_sem=e_send.at[k], recv_sem=e_recv.at[k],
            device_id=(g, sibling), device_id_type=MESH,
        )

    def pair(src, lo, hi, send, recv, i):
        def sem(sems, k):
            return sems.at[k] if i is None else sems.at[k, i]

        return (
            pltpu.make_async_remote_copy(
                src_ref=src, dst_ref=lo, send_sem=sem(send, 0), recv_sem=sem(recv, 0),
                device_id=(after, m), device_id_type=MESH,
            ),
            pltpu.make_async_remote_copy(
                src_ref=src, dst_ref=hi, send_sem=sem(send, 1), recv_sem=sem(recv, 1),
                device_id=(before, m), device_id_type=MESH,
            ),
        )

    def d_copies(d):
        return pair(od.at[:, cols(d)], lo_h.at[d], hi_h.at[d], d_send, d_recv, d)

    def g_pair(rows, send, recv, i):
        return pair(og.at[rows, :], glo.at[rows, :], ghi.at[rows, :], send, recv, i)

    def rest(i):
        return pl.ds(pl.multiple_of(AWAY + i * REST, 16), REST)

    def g_copies(i):
        return g_pair(rest(i), g_send, g_recv, i)

    def b_copies():
        return g_pair(rows_b, b_send, b_recv, None)

    def u_copies(i):
        rows = cols(i, ROWS)
        return pair(ou.at[rows, :], ulo.at[rows, :], uhi.at[rows, :], u_send, u_recv, i)

    def send(src, dst, send_sem, recv_sem, replica):
        return pltpu.make_async_remote_copy(
            src_ref=src, dst_ref=dst, send_sem=send_sem, recv_sem=recv_sem,
            device_id=(replica, m), device_id_type=MESH,
        )

    def relay_out():
        return send(od.at[early, cols(1)], relayed, relay_sem.at[0], relay_sem.at[1], far_end)

    def relay_over():
        return send(relayed, relayed, relay_sem.at[2], relay_sem.at[1], diagonal)

    def relay_on(first):
        dst, k, where = (lo_h, 0, before) if first else (hi_h, 1, after)
        return send(relayed, dst.at[1, early, :], relay_sem.at[2], d_recv.at[k, 1], where)

    def late_copies():
        return (
            send(od.at[late, cols(1)], lo_h.at[1, late, :], d_send.at[0, 1], d_recv.at[0, 1], after),
            send(od.at[late, cols(1)], hi_h.at[1, late, :], d_send.at[1, 1], d_recv.at[1, 1], before),
        )

    def cross_out(first):
        src, where = (glo, across_down) if first else (ghi, across_up)
        return send(src.at[rows_b, :], crossing, cross_sem.at[0], cross_sem.at[1], where)

    def cross_in(first):
        return send(crossing, summing, cross_sem.at[2], cross_sem.at[3], after if first else before)

    def cross_end(first):
        dst, where = (ghi, before) if first else (glo, after)
        return send(summing, dst.at[rows_b, :], cross_sem.at[4], cross_sem.at[5], where)

    def partial(d, carry):
        part[:, cols(d)] = dot(hid[...], wd[:, cols(d)], ((1,), (0,))).astype(BF16)

        @pl.when(d == 0)
        def _():
            for i in range(n_heads):
                p_copy(*head(i)).start()

        pl.when(d > 0)(p_copy(*block(d)).start)
        return carry

    def join(at, k):
        p_copy(at, k).wait()
        total = part[mine, at].astype(F32) + part_in[:, at].astype(F32)
        part[mine, at] = total.astype(BF16)
        straight = jnp.logical_or(k <= last, inside)
        pl.when(straight)(q_copy(at, k).start)
        pl.when(jnp.logical_not(straight))(detour_out(jnp.maximum(k - last - 1, 0)).start)

    def join_head(i, carry):
        join(*head(i))
        return carry

    def spread(d, carry):
        partial(d, carry)
        join(*block(d - 1))
        return carry

    lax.fori_loop(0, 2, partial, 0)
    lax.fori_loop(0, n_heads, join_head, 0)
    lax.fori_loop(2, n_cols, spread, 0)
    join(*block(n_cols - 1))

    def turn(i, carry):
        hid_t[cols(i), :] = hid[:, cols(i)].T
        return carry

    lax.fori_loop(0, n_units, turn, 0)

    def norm(i, carry):
        rows = cols(i, 64)
        nrm[rows, :] = (x[rows, :].astype(F32) * inv[rows, :]).astype(BF16)
        return carry

    tgt_copy.wait()

    def step_down(at, k):
        q_copy(at, k).wait()

        @pl.when(jnp.logical_and(at_end, k == last))
        def _():
            tell(go_sem, facing)

        total = part[mine, at].astype(F32) + sum_in[:, at].astype(F32)
        offset = x[mine, at].astype(F32) - tg[:, at].astype(F32)
        err[mine, at] = ((offset + total * mid_scale) / toks).astype(BF16)
        e_copy(at, k).start()
        e_copy(at, k).wait()
        grad = dot(hid_t[...], err[:, at], ((1,), (0,)))
        od[:, at] = (wd[:, at].astype(F32) - (step_size * mid_scale) * grad).astype(BF16)

    def inward_start(ahead, behind):
        pl.when(jnp.logical_not(last_end))(ahead.start)
        pl.when(jnp.logical_not(first_end))(behind.start)

    def down_head(i, carry):
        at, k = head(i)
        step_down(at, k)
        inward_start(
            *pair(od.at[:, at], lo_h.at[0, :, at], hi_h.at[0, :, at], d_send, d_recv, 0)
        )
        return carry

    def down(d, carry):
        @pl.when(jnp.logical_and(inside, d <= DETOUR))
        def _():
            i = jnp.minimum(d, DETOUR) - 1
            detour_out(i).wait_recv()
            detour_on(i).start()

        step_down(*block(d))

        @pl.when(d != 1)
        def _():
            inward_start(*d_copies(d))

        @pl.when(d == 1)
        def _():
            ahead, behind = d_copies(1)
            late_ahead, late_behind = late_copies()
            pl.when(along <= 1)(ahead.start)
            pl.when(along >= 2)(behind.start)
            pl.when(along == 2)(late_ahead.start)
            pl.when(along == 1)(late_behind.start)
            pl.when(at_end)(relay_out().start)

        return carry

    def down_late(d, carry):
        step_down(*block(d))
        for copy in d_copies(d):
            copy.start()
        return carry

    lax.fori_loop(0, n_heads, down_head, 0)
    lax.fori_loop(0, toks // 64, norm, 0)
    lax.fori_loop(1, n_cols - DETOUR, down, 0)

    @pl.when(at_end)
    def _():
        pl.semaphore_wait(go_sem, len(facing))

    def held_back(d, carry):
        ahead, behind = d_copies(d)
        pl.when(last_end)(ahead.start)
        pl.when(first_end)(behind.start)
        return carry

    held_back(0, 0)
    ahead, behind = late_copies()
    pl.when(last_end)(ahead.start)
    pl.when(first_end)(behind.start)
    lax.fori_loop(2, n_cols - DETOUR, held_back, 0)
    lax.fori_loop(n_cols - DETOUR, n_cols, down_late, 0)

    def back(f, carry):
        grad = dot(err[...], wd[cols(f), :], ((1,), (1,))) * mid_scale
        gg[:, cols(f)] = (grad * slope[:, cols(f)]).astype(BF16)
        gu[:, cols(f)] = (grad * act[:, cols(f)]).astype(BF16)
        return carry

    lax.fori_loop(0, n_units, back, 0)

    @pl.when(at_end)
    def _():
        relay_out().wait_recv()
        relay_over().start()

    def step(out, grads, rows):
        grad = dot(nrm[:, rows], grads[...], ((0,), (0,)))
        out[rows, :] = (out[rows, :].astype(F32) - (step_size * in_scale) * grad).astype(BF16)

    def step_up(i, carry):
        step(ou, gu, cols(i, ROWS))
        return carry

    def send_up(i, carry):
        for copy in u_copies(i):
            copy.start()
        return carry

    lower, upper = along <= 1, along >= 2
    first_in, last_in = along == 1, along == 2

    def step_gate(i, carry):
        step(og, gg, pl.ds(pl.multiple_of(i * 128, 128), 128))
        return carry

    def send_gate(i, carry):
        for copy in g_copies(i):
            copy.start()
        return carry

    lax.fori_loop(0, width // 128, step_gate, 0)
    ahead, behind = b_copies()
    pl.when(lower)(ahead.start)
    pl.when(upper)(behind.start)
    lax.fori_loop(0, n_rest, send_gate, 0)
    lax.fori_loop(0, n_rows, step_up, 0)

    def third(lo, own, hi):
        return ((lo.astype(F32) + own.astype(F32) + hi.astype(F32)) / 3.0).astype(BF16)

    def mix_down(d, carry):
        for copy in d_copies(d):
            copy.wait()
        loads = [
            pltpu.make_async_copy(lo_h.at[d], stage.at[0], st_sem.at[0]),
            pltpu.make_async_copy(hi_h.at[d], stage.at[1], st_sem.at[1]),
        ]
        for load in loads:
            load.start()
        for load in loads:
            load.wait()
        od[:, cols(d)] = third(stage[0], od[:, cols(d)], stage[1])
        return carry

    mix_down(0, 0)
    lax.fori_loop(2, n_cols, mix_down, 0)

    @pl.when(inside)
    def _():
        relay_out().wait_recv()
        both = relayed[...].astype(F32) + od[early, cols(1)].astype(F32)
        relayed[...] = both.astype(BF16)
        pl.when(first_in)(relay_on(True).start)
        pl.when(last_in)(relay_on(False).start)
        for copy in b_copies():
            copy.wait_recv()
        pl.when(first_in)(cross_out(True).start)
        pl.when(last_in)(cross_out(False).start)
        cross_out(True).wait_recv()
        pl.when(first_in)(cross_in(True).start)
        pl.when(last_in)(cross_in(False).start)

    lax.fori_loop(0, n_rows, send_up, 0)

    def mix(out, lo, hi, rows):
        out[rows, :] = third(lo[rows, :], out[rows, :], hi[rows, :])

    def mix_gate(i, carry):
        for copy in g_copies(i):
            copy.wait()
        mix(og, glo, ghi, rest(i))
        return carry

    lax.fori_loop(0, n_rest, mix_gate, 0)
    ahead, behind = d_copies(1)
    late_ahead, late_behind = late_copies()
    pl.when(lower)(ahead.wait_send)
    pl.when(upper)(behind.wait_send)
    pl.when(upper)(late_ahead.wait_send)
    pl.when(lower)(late_behind.wait_send)
    pl.when(at_end)(relay_out().wait_send)
    pl.when(jnp.logical_not(last_end))(ahead.wait_recv)
    pl.when(jnp.logical_not(first_end))(behind.wait_recv)
    pl.when(last_end)(late_ahead.wait_recv)
    pl.when(first_end)(late_behind.wait_recv)

    def load_second(rows, k):
        held = hi_h if k else lo_h
        return pltpu.make_async_copy(held.at[1, rows, :], stage.at[k, rows, :], st_sem.at[k])

    def third_second(rows):
        loads = [load_second(rows, k) for k in range(2)]
        for load in loads:
            load.start()
        for load in loads:
            load.wait()
        od[rows, cols(1)] = third(stage[0, rows, :], od[rows, cols(1)], stage[1, rows, :])

    third_second(late)

    @pl.when(inside)
    def _():
        third_second(early)

    def end(own, both):
        return ((own.astype(F32) + both.astype(F32)) / 3.0).astype(BF16)

    def end_second(k):
        load = load_second(early, k)
        load.start()
        load.wait()
        od[early, cols(1)] = end(od[early, cols(1)], stage[k, early, :])

    @pl.when(first_end)
    def _():
        end_second(0)

    @pl.when(last_end)
    def _():
        end_second(1)

    ahead, behind = b_copies()
    pl.when(lower)(ahead.wait_send)
    pl.when(upper)(behind.wait_send)

    @pl.when(inside)
    def _():
        cross_in(True).wait_recv()
        both = summing[...].astype(F32) + og[rows_b, :].astype(F32)
        summing[...] = both.astype(BF16)
        pl.when(first_in)(cross_end(True).start)
        pl.when(last_in)(cross_end(False).start)
        cross_out(True).wait_send()
        mix(og, glo, ghi, rows_b)

    def mix_up(i, carry):
        for copy in u_copies(i):
            copy.wait()
        mix(ou, ulo, uhi, cols(i, ROWS))
        return carry

    lax.fori_loop(0, n_rows, mix_up, 0)

    relay_over().wait_send()

    @pl.when(inside)
    def _():
        for i in range(DETOUR):
            detour_on(i).wait_send()

    @pl.when(inside)
    def _():
        cross_in(True).wait_send()
        cross_end(True).wait_send()

    @pl.when(first_end)
    def _():
        cross_end(True).wait_recv()
        og[rows_b, :] = end(og[rows_b, :], ghi[rows_b, :])

    @pl.when(last_end)
    def _():
        cross_end(False).wait_recv()
        og[rows_b, :] = end(og[rows_b, :], glo[rows_b, :])


def write_kernel(pieces, *refs):
    held, out, sem = refs[:3], refs[3:6], refs[6]
    copies = []
    for i in range(3):
        rows = held[i].shape[0] // pieces
        for p in range(pieces):
            part = pl.ds(p * rows, rows)
            copies.append(
                pltpu.make_async_copy(held[i].at[part, :], out[i].at[0, part, :], sem.at[i, p])
            )
    for copy in copies:
        copy.start()
    for copy in copies:
        copy.wait()


def write_out(*arrays):
    pieces = 4
    return pl.pallas_call(
        functools.partial(write_kernel, pieces),
        out_shape=tuple(jax.ShapeDtypeStruct((1, *a.shape), a.dtype) for a in arrays),
        in_specs=[pl.BlockSpec(memory_space=pltpu.VMEM)] * 3,
        out_specs=(pl.BlockSpec(memory_space=pl.ANY),) * 3,
        scratch_shapes=[pltpu.SemaphoreType.DMA((3, pieces))],
        compiler_params=pltpu.CompilerParams(vmem_limit_bytes=16 * 2**20),
    )(*arrays)


def local(replicas, tokens, targets, gate_weight, up_weight, down_weight):
    toks, width = tokens.shape[1:]
    units = gate_weight.shape[2]
    n_cols, n_rows, n_units = width // COLS, width // ROWS, units // COLS
    n_rest = (width - AWAY) // REST
    half = toks // 2
    dma = pltpu.SemaphoreType.DMA
    any_spec = pl.BlockSpec(memory_space=pl.ANY)
    vmem_spec = pl.BlockSpec(memory_space=pltpu.VMEM)
    received = jax.ShapeDtypeStruct((n_cols, units, COLS), BF16)
    gate_out, up_out, down_out, *_ = pl.pallas_call(
        functools.partial(kernel, replicas),
        out_shape=(
            pltpu.VMEM((width, units), BF16),
            pltpu.VMEM((width, units), BF16),
            pltpu.VMEM((units, width), BF16),
            received,
            received,
        ),
        in_specs=[any_spec] * 5,
        out_specs=(vmem_spec, vmem_spec, vmem_spec, any_spec, any_spec),
        scratch_shapes=[
            pltpu.VMEM((toks, width), BF16),
            pltpu.VMEM((half, width), BF16),
            pltpu.VMEM((toks, 1), F32),
            pltpu.VMEM((toks, width), BF16),
            pltpu.VMEM((units, width), BF16),
            pltpu.VMEM((toks, units), F32),
            pltpu.VMEM((toks, units), F32),
            pltpu.VMEM((toks, units), BF16),
            pltpu.VMEM((units, toks), BF16),
            pltpu.VMEM((toks, width), BF16),
            pltpu.VMEM((toks, units), BF16),
            pltpu.VMEM((toks, units), BF16),
            pltpu.VMEM((toks, width), BF16),
            pltpu.VMEM((half, width), BF16),
            pltpu.VMEM((half, width), BF16),
            pltpu.VMEM((DETOUR, half, COLS), BF16),
            pltpu.VMEM((width, units), BF16),
            pltpu.VMEM((width, units), BF16),
            pltpu.VMEM((width, units), BF16),
            pltpu.VMEM((width, units), BF16),
            pltpu.VMEM((2, units, COLS), BF16),
            pltpu.VMEM((AWAY, units), BF16),
            pltpu.VMEM((AWAY, units), BF16),
            pltpu.VMEM((FIRST, COLS), BF16),
            dma((4,)),
            dma((2,)),
            dma((2, n_units)),
            dma((n_cols + COLS // HEAD - 1,)),
            dma((n_cols + COLS // HEAD - 1,)),
            dma((n_cols + COLS // HEAD - 1,)),
            dma((n_cols + COLS // HEAD - 1,)),
            dma((n_cols + COLS // HEAD - 1,)),
            dma((n_cols + COLS // HEAD - 1,)),
            dma((2, n_cols)),
            dma((2, n_cols)),
            dma((2, n_rest)),
            dma((2, n_rest)),
            dma((2, n_rows)),
            dma((2, n_rows)),
            dma((2,)),
            dma((2,)),
            dma((2,)),
            dma((3,)),
            dma((6,)),
            dma((2, DETOUR)),
            pltpu.SemaphoreType.REGULAR,
        ],
        compiler_params=pltpu.CompilerParams(
            collective_id=0, has_side_effects=True, vmem_limit_bytes=50 * 2**20
        ),
    )(tokens[0], targets[0], gate_weight[0], up_weight[0], down_weight[0])
    return write_out(gate_out, up_out, down_out)


def solution(mesh):
    placed = (
        P("gossip", None, None),
        P("gossip", None, None),
        P("gossip", None, "mp"),
        P("gossip", None, "mp"),
        P("gossip", "mp", None),
    )
    return jax.shard_map(
        functools.partial(local, mesh.shape["gossip"]),
        mesh=mesh,
        in_specs=placed,
        out_specs=(P("gossip", None, "mp"), P("gossip", None, "mp"), P("gossip", "mp", None)),
        check_vma=False,
    )
```

```python
import functools

import jax
import jax.numpy as jnp
from jax import lax
from jax.experimental import pallas as pl
from jax.experimental.pallas import tpu as pltpu
from jax.sharding import PartitionSpec as P

MESH = pl.DeviceIdType.MESH
F32 = jnp.float32
BF16 = jnp.bfloat16
COLS = 256
X, Y = 4, 2
ROWS = 256
REST = 208
AWAY = 176
FIRST = 448
DETOUR = 2
HEAD = 128


def dot(a, b, dims):
    return lax.dot_general(a, b, (dims, ((), ())), preferred_element_type=F32)


def kernel(
    replicas,
    tok_h, tgt_h, wg_h, wu_h, wd_h,
    og, ou, od, lo_h, hi_h,
    x, tg, inv, nrm, wd, slope, act, hid, hid_t, err, gg, gu,
    part, part_in, sum_in, passing, glo, ghi, ulo, uhi, stage, crossing, summing, relayed,
    tok_sem, load_sem, w_sem, p_send, p_recv, q_send, q_recv, e_send, e_recv,
    d_send, d_recv, g_send, g_recv, u_send, u_recv, st_sem,
    b_send, b_recv, relay_sem, cross_sem, pass_sem, go_sem,
):
    g = lax.axis_index("gossip")
    m = lax.axis_index("mp")
    core = lax.rem(m, 2)
    sibling = m + 1 - 2 * core
    peer = lax.rem(m + 2, 4)
    after = lax.rem(g + 1, replicas)
    before = lax.rem(g + replicas - 1, replicas)
    toks, width = x.shape
    units = wd.shape[0]
    half = toks // 2
    in_scale = 1.0 / width**0.5
    mid_scale = 1.0 / (4 * units) ** 0.5
    step_size = (4 * units) / 4.0

    def cols(i, size=COLS):
        return pl.ds(pl.multiple_of(i * size, size), size)

    n_cols = width // COLS
    n_rows = width // ROWS
    n_rest = (width - AWAY) // REST
    rows_b = pl.ds(0, AWAY)
    early, late = pl.ds(0, FIRST), pl.ds(FIRST, units - FIRST)
    n_units = units // COLS
    mine = pl.ds(pl.multiple_of(core * half, half), half)
    theirs = pl.ds(pl.multiple_of((1 - core) * half, half), half)

    piece = toks // 4

    def tok_copy(i):
        rows = cols(i, piece)
        return pltpu.make_async_copy(tok_h.at[rows, :], x.at[rows, :], tok_sem.at[i])

    for i in range(4):
        tok_copy(i).start()

    def w_copies(f):
        return (
            pltpu.make_async_copy(wg_h.at[:, cols(f)], og.at[:, cols(f)], w_sem.at[0, f]),
            pltpu.make_async_copy(wu_h.at[:, cols(f)], ou.at[:, cols(f)], w_sem.at[1, f]),
        )

    for copy in w_copies(0):
        copy.start()

    wd_copy = pltpu.make_async_copy(wd_h, wd, load_sem.at[0])
    tgt_copy = pltpu.make_async_copy(tgt_h.at[mine, :], tg, load_sem.at[1])

    along = lax.rem(g, X)
    last_end = along == X - 1
    first_end = along == 0
    at_end = jnp.logical_or(last_end, first_end)
    layer = g // (X * Y)
    layers = replicas // (X * Y)
    beyond = lax.rem(layer + (along // (X - 1)) * 2 - 1 + layers, layers)
    facing = [
        (at * (X * Y) + row * X + (X - 1 - along), shard)
        for at in (layer, beyond)
        for row in range(Y)
        for shard in range(4)
    ]

    def tell(sem, wheres):
        for where in wheres:
            pl.semaphore_signal(sem, inc=1, device_id=where, device_id_type=MESH)

    barrier = pltpu.get_barrier_semaphore()
    far_end = g + (X - 1) * (1 - 2 * (along // (X - 1)))
    diagonal = lax.rem(g + (X + 1) * (1 - 2 * lax.rem(along, 2)) + replicas, replicas)
    across_up = lax.rem(g + X, replicas)
    across_down = lax.rem(g - X + replicas, replicas)
    beside = g + 1 - 2 * lax.rem(along, 2)
    near = ((g, sibling), (g, peer), (diagonal, m), (beside, peer))
    inward = g + 1 - 2 * (along // (X - 1))

    @pl.when(jnp.logical_not(at_end))
    def _():
        tell(barrier, (*near, (after, m), (before, m), (across_up, m), (across_down, m)))

    @pl.when(at_end)
    def _():
        tell(barrier, (*near, (inward, m), *facing))

    def square(i, carry):
        rows = cols(i, 64)
        wide = x[rows, :].astype(F32)
        mean = jnp.mean(wide * wide, axis=-1, keepdims=True)
        inv[rows, :] = lax.rsqrt(mean + 1e-06)
        return carry

    for i in range(4):
        tok_copy(i).wait()
        lax.fori_loop(i * piece // 64, (i + 1) * piece // 64, square, 0)
        for copy in w_copies(i + 1) if i + 1 < n_units else (wd_copy, tgt_copy):
            copy.start()

    def forward(f, carry):
        for copy in w_copies(f):
            copy.wait()
        scale = inv[...] * in_scale
        gate = dot(x[...], og[:, cols(f)], ((1,), (0,))) * scale
        up = dot(x[...], ou[:, cols(f)], ((1,), (0,))) * scale
        sig = jax.nn.sigmoid(gate)
        acted = gate * sig
        act[:, cols(f)] = acted
        slope[:, cols(f)] = up * (sig * (1.0 + gate * (1.0 - sig)))
        hid[:, cols(f)] = (acted * up).astype(BF16)
        return carry

    lax.fori_loop(0, n_units, forward, 0)
    wd_copy.wait()

    @pl.when(jnp.logical_not(at_end))
    def _():
        pl.semaphore_wait(barrier, len(near) + 4)

    @pl.when(at_end)
    def _():
        pl.semaphore_wait(barrier, len(near) + 1 + len(facing))

    def head(i):
        return cols(i, HEAD), i

    def block(d):
        return cols(d), d + COLS // HEAD - 1

    n_heads = COLS // HEAD
    last = n_cols + n_heads - 2 - DETOUR
    inside = jnp.logical_not(at_end)

    def p_copy(at, k):
        return pltpu.make_async_remote_copy(
            src_ref=part.at[theirs, at], dst_ref=part_in.at[:, at],
            send_sem=p_send.at[k], recv_sem=p_recv.at[k],
            device_id=(g, sibling), device_id_type=MESH,
        )

    def q_copy(at, k):
        return pltpu.make_async_remote_copy(
            src_ref=part.at[mine, at], dst_ref=sum_in.at[:, at],
            send_sem=q_send.at[k], recv_sem=q_recv.at[k],
            device_id=(g, peer), device_id_type=MESH,
        )

    def detour_out(i):
        d = n_cols - DETOUR + i
        return pltpu.make_async_remote_copy(
            src_ref=part.at[mine, cols(d)], dst_ref=passing.at[i],
            send_sem=q_send.at[block(d)[1]], recv_sem=pass_sem.at[0, i],
            device_id=(beside, peer), device_id_type=MESH,
        )

    def detour_on(i):
        d = n_cols - DETOUR + i
        return pltpu.make_async_remote_copy(
            src_ref=passing.at[i], dst_ref=sum_in.at[:, cols(d)],
            send_sem=pass_sem.at[1, i], recv_sem=q_recv.at[block(d)[1]],
            device_id=(beside, m), device_id_type=MESH,
        )

    def e_copy(at, k):
        return pltpu.make_async_remote_copy(
            src_ref=err.at[mine, at], dst_ref=err.at[mine, at],
            send_sem=e_send.at[k], recv_sem=e_recv.at[k],
            device_id=(g, sibling), device_id_type=MESH,
        )

    def pair(src, lo, hi, send, recv, i):
        def sem(sems, k):
            return sems.at[k] if i is None else sems.at[k, i]

        return (
            pltpu.make_async_remote_copy(
                src_ref=src, dst_ref=lo, send_sem=sem(send, 0), recv_sem=sem(recv, 0),
                device_id=(after, m), device_id_type=MESH,
            ),
            pltpu.make_async_remote_copy(
                src_ref=src, dst_ref=hi, send_sem=sem(send, 1), recv_sem=sem(recv, 1),
                device_id=(before, m), device_id_type=MESH,
            ),
        )

    def d_copies(d):
        return pair(od.at[:, cols(d)], lo_h.at[d], hi_h.at[d], d_send, d_recv, d)

    def g_pair(rows, send, recv, i):
        return pair(og.at[rows, :], glo.at[rows, :], ghi.at[rows, :], send, recv, i)

    def rest(i):
        return pl.ds(pl.multiple_of(AWAY + i * REST, 16), REST)

    def g_copies(i):
        return g_pair(rest(i), g_send, g_recv, i)

    def b_copies():
        return g_pair(rows_b, b_send, b_recv, None)

    def u_copies(i):
        rows = cols(i, ROWS)
        return pair(ou.at[rows, :], ulo.at[rows, :], uhi.at[rows, :], u_send, u_recv, i)

    def send(src, dst, send_sem, recv_sem, replica):
        return pltpu.make_async_remote_copy(
            src_ref=src, dst_ref=dst, send_sem=send_sem, recv_sem=recv_sem,
            device_id=(replica, m), device_id_type=MESH,
        )

    def relay_out():
        return send(od.at[early, cols(1)], relayed, relay_sem.at[0], relay_sem.at[1], far_end)

    def relay_over():
        return send(relayed, relayed, relay_sem.at[2], relay_sem.at[1], diagonal)

    def relay_on(first):
        dst, k, where = (lo_h, 0, before) if first else (hi_h, 1, after)
        return send(relayed, dst.at[1, early, :], relay_sem.at[2], d_recv.at[k, 1], where)

    def late_copies():
        return (
            send(od.at[late, cols(1)], lo_h.at[1, late, :], d_send.at[0, 1], d_recv.at[0, 1], after),
            send(od.at[late, cols(1)], hi_h.at[1, late, :], d_send.at[1, 1], d_recv.at[1, 1], before),
        )

    def cross_out(first):
        src, where = (glo, across_down) if first else (ghi, across_up)
        return send(src.at[rows_b, :], crossing, cross_sem.at[0], cross_sem.at[1], where)

    def cross_in(first):
        return send(crossing, summing, cross_sem.at[2], cross_sem.at[3], after if first else before)

    def cross_end(first):
        dst, where = (ghi, before) if first else (glo, after)
        return send(summing, dst.at[rows_b, :], cross_sem.at[4], cross_sem.at[5], where)

    def partial(d, carry):
        part[:, cols(d)] = dot(hid[...], wd[:, cols(d)], ((1,), (0,))).astype(BF16)

        @pl.when(d == 0)
        def _():
            for i in range(n_heads):
                p_copy(*head(i)).start()

        pl.when(d > 0)(p_copy(*block(d)).start)
        return carry

    def join(at, k):
        p_copy(at, k).wait()
        total = part[mine, at].astype(F32) + part_in[:, at].astype(F32)
        part[mine, at] = total.astype(BF16)
        straight = jnp.logical_or(k <= last, inside)
        pl.when(straight)(q_copy(at, k).start)
        pl.when(jnp.logical_not(straight))(detour_out(jnp.maximum(k - last - 1, 0)).start)

    def join_head(i, carry):
        join(*head(i))
        return carry

    def spread(d, carry):
        partial(d, carry)
        join(*block(d - 1))
        return carry

    lax.fori_loop(0, 2, partial, 0)
    lax.fori_loop(0, n_heads, join_head, 0)
    lax.fori_loop(2, n_cols, spread, 0)
    join(*block(n_cols - 1))

    def turn(i, carry):
        hid_t[cols(i), :] = hid[:, cols(i)].T
        return carry

    lax.fori_loop(0, n_units, turn, 0)

    def norm(i, carry):
        rows = cols(i, 64)
        nrm[rows, :] = (x[rows, :].astype(F32) * inv[rows, :]).astype(BF16)
        return carry

    tgt_copy.wait()

    def step_down(at, k):
        q_copy(at, k).wait()

        @pl.when(jnp.logical_and(at_end, k == last))
        def _():
            tell(go_sem, facing)

        total = part[mine, at].astype(F32) + sum_in[:, at].astype(F32)
        offset = x[mine, at].astype(F32) - tg[:, at].astype(F32)
        err[mine, at] = ((offset + total * mid_scale) / toks).astype(BF16)
        e_copy(at, k).start()
        e_copy(at, k).wait()
        grad = dot(hid_t[...], err[:, at], ((1,), (0,)))
        od[:, at] = (wd[:, at].astype(F32) - (step_size * mid_scale) * grad).astype(BF16)

    def inward_start(ahead, behind):
        pl.when(jnp.logical_not(last_end))(ahead.start)
        pl.when(jnp.logical_not(first_end))(behind.start)

    def down_head(i, carry):
        at, k = head(i)
        step_down(at, k)
        inward_start(
            *pair(od.at[:, at], lo_h.at[0, :, at], hi_h.at[0, :, at], d_send, d_recv, 0)
        )
        return carry

    def down(d, carry):
        @pl.when(jnp.logical_and(inside, jnp.logical_and(d >= 2, d < 2 + DETOUR)))
        def _():
            i = lax.rem(d + DETOUR - 2, DETOUR)
            detour_out(i).wait_recv()
            detour_on(i).start()

        step_down(*block(d))

        @pl.when(d != 1)
        def _():
            inward_start(*d_copies(d))

        @pl.when(d == 1)
        def _():
            ahead, behind = d_copies(1)
            late_ahead, late_behind = late_copies()
            pl.when(along <= 1)(ahead.start)
            pl.when(along >= 2)(behind.start)
            pl.when(along == 2)(late_ahead.start)
            pl.when(along == 1)(late_behind.start)
            pl.when(at_end)(relay_out().start)

        return carry

    def down_late(d, carry):
        step_down(*block(d))
        for copy in d_copies(d):
            copy.start()
        return carry

    lax.fori_loop(0, n_heads, down_head, 0)
    lax.fori_loop(0, toks // 64, norm, 0)
    lax.fori_loop(1, n_cols - DETOUR, down, 0)

    @pl.when(at_end)
    def _():
        pl.semaphore_wait(go_sem, len(facing))

    def held_back(d, carry):
        ahead, behind = d_copies(d)
        pl.when(last_end)(ahead.start)
        pl.when(first_end)(behind.start)
        return carry

    held_back(0, 0)
    ahead, behind = late_copies()
    pl.when(last_end)(ahead.start)
    pl.when(first_end)(behind.start)
    lax.fori_loop(2, n_cols - DETOUR, held_back, 0)
    lax.fori_loop(n_cols - DETOUR, n_cols, down_late, 0)

    def back(f, carry):
        grad = dot(err[...], wd[cols(f), :], ((1,), (1,))) * mid_scale
        gg[:, cols(f)] = (grad * slope[:, cols(f)]).astype(BF16)
        gu[:, cols(f)] = (grad * act[:, cols(f)]).astype(BF16)
        return carry

    lax.fori_loop(0, n_units, back, 0)

    @pl.when(at_end)
    def _():
        relay_out().wait_recv()
        relay_over().start()

    def step(out, grads, rows):
        grad = dot(nrm[:, rows], grads[...], ((0,), (0,)))
        out[rows, :] = (out[rows, :].astype(F32) - (step_size * in_scale) * grad).astype(BF16)

    def step_up(i, carry):
        step(ou, gu, cols(i, ROWS))
        return carry

    def send_up(i, carry):
        for copy in u_copies(i):
            copy.start()
        return carry

    lower, upper = along <= 1, along >= 2
    first_in, last_in = along == 1, along == 2

    def step_gate(i, carry):
        step(og, gg, pl.ds(pl.multiple_of(i * 128, 128), 128))
        return carry

    def send_gate(i, carry):
        for copy in g_copies(i):
            copy.start()
        return carry

    lax.fori_loop(0, width // 128, step_gate, 0)
    ahead, behind = b_copies()
    pl.when(lower)(ahead.start)
    pl.when(upper)(behind.start)
    lax.fori_loop(0, n_rest, send_gate, 0)
    lax.fori_loop(0, n_rows, step_up, 0)

    def third(lo, own, hi):
        return ((lo.astype(F32) + own.astype(F32) + hi.astype(F32)) / 3.0).astype(BF16)

    def mix_down(d, carry):
        for copy in d_copies(d):
            copy.wait()
        loads = [
            pltpu.make_async_copy(lo_h.at[d], stage.at[0], st_sem.at[0]),
            pltpu.make_async_copy(hi_h.at[d], stage.at[1], st_sem.at[1]),
        ]
        for load in loads:
            load.start()
        for load in loads:
            load.wait()
        od[:, cols(d)] = third(stage[0], od[:, cols(d)], stage[1])
        return carry

    mix_down(0, 0)
    lax.fori_loop(2, n_cols, mix_down, 0)

    @pl.when(inside)
    def _():
        relay_out().wait_recv()
        both = relayed[...].astype(F32) + od[early, cols(1)].astype(F32)
        relayed[...] = both.astype(BF16)
        pl.when(first_in)(relay_on(True).start)
        pl.when(last_in)(relay_on(False).start)
        for copy in b_copies():
            copy.wait_recv()
        pl.when(first_in)(cross_out(True).start)
        pl.when(last_in)(cross_out(False).start)
        cross_out(True).wait_recv()
        pl.when(first_in)(cross_in(True).start)
        pl.when(last_in)(cross_in(False).start)

    lax.fori_loop(0, n_rows, send_up, 0)

    def mix(out, lo, hi, rows):
        out[rows, :] = third(lo[rows, :], out[rows, :], hi[rows, :])

    def mix_gate(i, carry):
        for copy in g_copies(i):
            copy.wait()
        mix(og, glo, ghi, rest(i))
        return carry

    lax.fori_loop(0, n_rest, mix_gate, 0)
    ahead, behind = d_copies(1)
    late_ahead, late_behind = late_copies()
    pl.when(lower)(ahead.wait_send)
    pl.when(upper)(behind.wait_send)
    pl.when(upper)(late_ahead.wait_send)
    pl.when(lower)(late_behind.wait_send)
    pl.when(at_end)(relay_out().wait_send)
    pl.when(jnp.logical_not(last_end))(ahead.wait_recv)
    pl.when(jnp.logical_not(first_end))(behind.wait_recv)
    pl.when(last_end)(late_ahead.wait_recv)
    pl.when(first_end)(late_behind.wait_recv)

    def load_second(rows, k):
        held = hi_h if k else lo_h
        return pltpu.make_async_copy(held.at[1, rows, :], stage.at[k, rows, :], st_sem.at[k])

    def third_second(rows):
        loads = [load_second(rows, k) for k in range(2)]
        for load in loads:
            load.start()
        for load in loads:
            load.wait()
        od[rows, cols(1)] = third(stage[0, rows, :], od[rows, cols(1)], stage[1, rows, :])

    third_second(late)

    @pl.when(inside)
    def _():
        third_second(early)

    def end(own, both):
        return ((own.astype(F32) + both.astype(F32)) / 3.0).astype(BF16)

    def end_second(k):
        load = load_second(early, k)
        load.start()
        load.wait()
        od[early, cols(1)] = end(od[early, cols(1)], stage[k, early, :])

    @pl.when(first_end)
    def _():
        end_second(0)

    @pl.when(last_end)
    def _():
        end_second(1)

    ahead, behind = b_copies()
    pl.when(lower)(ahead.wait_send)
    pl.when(upper)(behind.wait_send)

    @pl.when(inside)
    def _():
        cross_in(True).wait_recv()
        both = summing[...].astype(F32) + og[rows_b, :].astype(F32)
        summing[...] = both.astype(BF16)
        pl.when(first_in)(cross_end(True).start)
        pl.when(last_in)(cross_end(False).start)
        cross_out(True).wait_send()
        mix(og, glo, ghi, rows_b)

    def mix_up(i, carry):
        for copy in u_copies(i):
            copy.wait()
        mix(ou, ulo, uhi, cols(i, ROWS))
        return carry

    lax.fori_loop(0, n_rows, mix_up, 0)

    relay_over().wait_send()

    @pl.when(inside)
    def _():
        for i in range(DETOUR):
            detour_on(i).wait_send()

    @pl.when(inside)
    def _():
        cross_in(True).wait_send()
        cross_end(True).wait_send()

    @pl.when(first_end)
    def _():
        cross_end(True).wait_recv()
        og[rows_b, :] = end(og[rows_b, :], ghi[rows_b, :])

    @pl.when(last_end)
    def _():
        cross_end(False).wait_recv()
        og[rows_b, :] = end(og[rows_b, :], glo[rows_b, :])


def write_kernel(pieces, *refs):
    held, out, sem = refs[:3], refs[3:6], refs[6]
    copies = []
    for i in range(3):
        rows = held[i].shape[0] // pieces
        for p in range(pieces):
            part = pl.ds(p * rows, rows)
            copies.append(
                pltpu.make_async_copy(held[i].at[part, :], out[i].at[0, part, :], sem.at[i, p])
            )
    for copy in copies:
        copy.start()
    for copy in copies:
        copy.wait()


def write_out(*arrays):
    pieces = 4
    return pl.pallas_call(
        functools.partial(write_kernel, pieces),
        out_shape=tuple(jax.ShapeDtypeStruct((1, *a.shape), a.dtype) for a in arrays),
        in_specs=[pl.BlockSpec(memory_space=pltpu.VMEM)] * 3,
        out_specs=(pl.BlockSpec(memory_space=pl.ANY),) * 3,
        scratch_shapes=[pltpu.SemaphoreType.DMA((3, pieces))],
        compiler_params=pltpu.CompilerParams(vmem_limit_bytes=16 * 2**20),
    )(*arrays)


def local(replicas, tokens, targets, gate_weight, up_weight, down_weight):
    toks, width = tokens.shape[1:]
    units = gate_weight.shape[2]
    n_cols, n_rows, n_units = width // COLS, width // ROWS, units // COLS
    n_rest = (width - AWAY) // REST
    half = toks // 2
    dma = pltpu.SemaphoreType.DMA
    any_spec = pl.BlockSpec(memory_space=pl.ANY)
    vmem_spec = pl.BlockSpec(memory_space=pltpu.VMEM)
    received = jax.ShapeDtypeStruct((n_cols, units, COLS), BF16)
    gate_out, up_out, down_out, *_ = pl.pallas_call(
        functools.partial(kernel, replicas),
        out_shape=(
            pltpu.VMEM((width, units), BF16),
            pltpu.VMEM((width, units), BF16),
            pltpu.VMEM((units, width), BF16),
            received,
            received,
        ),
        in_specs=[any_spec] * 5,
        out_specs=(vmem_spec, vmem_spec, vmem_spec, any_spec, any_spec),
        scratch_shapes=[
            pltpu.VMEM((toks, width), BF16),
            pltpu.VMEM((half, width), BF16),
            pltpu.VMEM((toks, 1), F32),
            pltpu.VMEM((toks, width), BF16),
            pltpu.VMEM((units, width), BF16),
            pltpu.VMEM((toks, units), F32),
            pltpu.VMEM((toks, units), F32),
            pltpu.VMEM((toks, units), BF16),
            pltpu.VMEM((units, toks), BF16),
            pltpu.VMEM((toks, width), BF16),
            pltpu.VMEM((toks, units), BF16),
            pltpu.VMEM((toks, units), BF16),
            pltpu.VMEM((toks, width), BF16),
            pltpu.VMEM((half, width), BF16),
            pltpu.VMEM((half, width), BF16),
            pltpu.VMEM((DETOUR, half, COLS), BF16),
            pltpu.VMEM((width, units), BF16),
            pltpu.VMEM((width, units), BF16),
            pltpu.VMEM((width, units), BF16),
            pltpu.VMEM((width, units), BF16),
            pltpu.VMEM((2, units, COLS), BF16),
            pltpu.VMEM((AWAY, units), BF16),
            pltpu.VMEM((AWAY, units), BF16),
            pltpu.VMEM((FIRST, COLS), BF16),
            dma((4,)),
            dma((2,)),
            dma((2, n_units)),
            dma((n_cols + COLS // HEAD - 1,)),
            dma((n_cols + COLS // HEAD - 1,)),
            dma((n_cols + COLS // HEAD - 1,)),
            dma((n_cols + COLS // HEAD - 1,)),
            dma((n_cols + COLS // HEAD - 1,)),
            dma((n_cols + COLS // HEAD - 1,)),
            dma((2, n_cols)),
            dma((2, n_cols)),
            dma((2, n_rest)),
            dma((2, n_rest)),
            dma((2, n_rows)),
            dma((2, n_rows)),
            dma((2,)),
            dma((2,)),
            dma((2,)),
            dma((3,)),
            dma((6,)),
            dma((2, DETOUR)),
            pltpu.SemaphoreType.REGULAR,
        ],
        compiler_params=pltpu.CompilerParams(
            collective_id=0, has_side_effects=True, vmem_limit_bytes=50 * 2**20
        ),
    )(tokens[0], targets[0], gate_weight[0], up_weight[0], down_weight[0])
    return write_out(gate_out, up_out, down_out)


def solution(mesh):
    placed = (
        P("gossip", None, None),
        P("gossip", None, None),
        P("gossip", None, "mp"),
        P("gossip", None, "mp"),
        P("gossip", "mp", None),
    )
    return jax.shard_map(
        functools.partial(local, mesh.shape["gossip"]),
        mesh=mesh,
        in_specs=placed,
        out_specs=(P("gossip", None, "mp"), P("gossip", None, "mp"), P("gossip", "mp", None)),
        check_vma=False,
    )
```

```python
import functools

import jax
import jax.numpy as jnp
from jax import lax
from jax.experimental import pallas as pl
from jax.experimental.pallas import tpu as pltpu
from jax.sharding import PartitionSpec as P

MESH = pl.DeviceIdType.MESH
F32 = jnp.float32
BF16 = jnp.bfloat16
COLS = 256
X, Y = 4, 2
ROWS = 256
REST = 208
AWAY = 176
FIRST = 448
DETOUR = 2
HEAD = 128


def dot(a, b, dims):
    return lax.dot_general(a, b, (dims, ((), ())), preferred_element_type=F32)


def kernel(
    replicas,
    tok_h, tgt_h, wg_h, wu_h, wd_h,
    og, ou, od, lo_h, hi_h,
    x, tg, inv, nrm, wd, slope, act, hid, hid_t, err, gg, gu,
    part, part_in, sum_in, passing, glo, ghi, ulo, uhi, stage, crossing, summing, relayed,
    tok_sem, load_sem, w_sem, p_send, p_recv, q_send, q_recv, e_send, e_recv,
    d_send, d_recv, g_send, g_recv, u_send, u_recv, st_sem,
    b_send, b_recv, relay_sem, cross_sem, pass_sem, go_sem,
):
    g = lax.axis_index("gossip")
    m = lax.axis_index("mp")
    core = lax.rem(m, 2)
    sibling = m + 1 - 2 * core
    peer = lax.rem(m + 2, 4)
    after = lax.rem(g + 1, replicas)
    before = lax.rem(g + replicas - 1, replicas)
    toks, width = x.shape
    units = wd.shape[0]
    half = toks // 2
    in_scale = 1.0 / width**0.5
    mid_scale = 1.0 / (4 * units) ** 0.5
    step_size = (4 * units) / 4.0

    def cols(i, size=COLS):
        return pl.ds(pl.multiple_of(i * size, size), size)

    n_cols = width // COLS
    n_rows = width // ROWS
    n_rest = (width - AWAY) // REST
    rows_b = pl.ds(0, AWAY)
    early, late = pl.ds(0, FIRST), pl.ds(FIRST, units - FIRST)
    n_units = units // COLS
    mine = pl.ds(pl.multiple_of(core * half, half), half)
    theirs = pl.ds(pl.multiple_of((1 - core) * half, half), half)

    piece = toks // 4

    def tok_copy(i):
        rows = cols(i, piece)
        return pltpu.make_async_copy(tok_h.at[rows, :], x.at[rows, :], tok_sem.at[i])

    for i in range(4):
        tok_copy(i).start()

    def w_copies(f):
        return (
            pltpu.make_async_copy(wg_h.at[:, cols(f)], og.at[:, cols(f)], w_sem.at[0, f]),
            pltpu.make_async_copy(wu_h.at[:, cols(f)], ou.at[:, cols(f)], w_sem.at[1, f]),
        )

    for copy in w_copies(0):
        copy.start()

    wd_copy = pltpu.make_async_copy(wd_h, wd, load_sem.at[0])
    tgt_copy = pltpu.make_async_copy(tgt_h.at[mine, :], tg, load_sem.at[1])

    along = lax.rem(g, X)
    last_end = along == X - 1
    first_end = along == 0
    at_end = jnp.logical_or(last_end, first_end)
    layer = g // (X * Y)
    layers = replicas // (X * Y)
    beyond = lax.rem(layer + (along // (X - 1)) * 2 - 1 + layers, layers)
    facing = [
        (at * (X * Y) + row * X + (X - 1 - along), shard)
        for at in (layer, beyond)
        for row in range(Y)
        for shard in range(4)
    ]

    def tell(sem, wheres):
        for where in wheres:
            pl.semaphore_signal(sem, inc=1, device_id=where, device_id_type=MESH)

    barrier = pltpu.get_barrier_semaphore()
    far_end = g + (X - 1) * (1 - 2 * (along // (X - 1)))
    diagonal = lax.rem(g + (X + 1) * (1 - 2 * lax.rem(along, 2)) + replicas, replicas)
    across_up = lax.rem(g + X, replicas)
    across_down = lax.rem(g - X + replicas, replicas)
    beside = g + 1 - 2 * lax.rem(along, 2)
    near = ((g, sibling), (g, peer), (diagonal, m), (beside, peer))
    inward = g + 1 - 2 * (along // (X - 1))

    @pl.when(jnp.logical_not(at_end))
    def _():
        tell(barrier, (*near, (after, m), (before, m), (across_up, m), (across_down, m)))

    @pl.when(at_end)
    def _():
        tell(barrier, (*near, (inward, m), *facing))

    def square(i, carry):
        rows = cols(i, 64)
        wide = x[rows, :].astype(F32)
        mean = jnp.mean(wide * wide, axis=-1, keepdims=True)
        inv[rows, :] = lax.rsqrt(mean + 1e-06)
        return carry

    for i in range(4):
        tok_copy(i).wait()
        lax.fori_loop(i * piece // 64, (i + 1) * piece // 64, square, 0)
        for copy in w_copies(i + 1) if i + 1 < n_units else (wd_copy, tgt_copy):
            copy.start()

    def forward(f, carry):
        for copy in w_copies(f):
            copy.wait()
        scale = inv[...] * in_scale
        gate = dot(x[...], og[:, cols(f)], ((1,), (0,))) * scale
        up = dot(x[...], ou[:, cols(f)], ((1,), (0,))) * scale
        sig = jax.nn.sigmoid(gate)
        acted = gate * sig
        act[:, cols(f)] = acted
        slope[:, cols(f)] = up * (sig * (1.0 + gate * (1.0 - sig)))
        hid[:, cols(f)] = (acted * up).astype(BF16)
        return carry

    lax.fori_loop(0, n_units, forward, 0)
    wd_copy.wait()

    @pl.when(jnp.logical_not(at_end))
    def _():
        pl.semaphore_wait(barrier, len(near) + 4)

    @pl.when(at_end)
    def _():
        pl.semaphore_wait(barrier, len(near) + 1 + len(facing))

    def head(i):
        return cols(i, HEAD), i

    def block(d):
        return cols(d), d + COLS // HEAD - 1

    n_heads = COLS // HEAD
    last = n_cols + n_heads - 2 - DETOUR
    inside = jnp.logical_not(at_end)

    def p_copy(at, k):
        return pltpu.make_async_remote_copy(
            src_ref=part.at[theirs, at], dst_ref=part_in.at[:, at],
            send_sem=p_send.at[k], recv_sem=p_recv.at[k],
            device_id=(g, sibling), device_id_type=MESH,
        )

    def q_copy(at, k):
        return pltpu.make_async_remote_copy(
            src_ref=part.at[mine, at], dst_ref=sum_in.at[:, at],
            send_sem=q_send.at[k], recv_sem=q_recv.at[k],
            device_id=(g, peer), device_id_type=MESH,
        )

    def detour_out(i):
        d = n_cols - DETOUR + i
        return pltpu.make_async_remote_copy(
            src_ref=part.at[mine, cols(d)], dst_ref=passing.at[i],
            send_sem=q_send.at[block(d)[1]], recv_sem=pass_sem.at[0, i],
            device_id=(beside, peer), device_id_type=MESH,
        )

    def detour_on(i):
        d = n_cols - DETOUR + i
        return pltpu.make_async_remote_copy(
            src_ref=passing.at[i], dst_ref=sum_in.at[:, cols(d)],
            send_sem=pass_sem.at[1, i], recv_sem=q_recv.at[block(d)[1]],
            device_id=(beside, m), device_id_type=MESH,
        )

    def e_copy(at, k):
        return pltpu.make_async_remote_copy(
            src_ref=err.at[mine, at], dst_ref=err.at[mine, at],
            send_sem=e_send.at[k], recv_sem=e_recv.at[k],
            device_id=(g, sibling), device_id_type=MESH,
        )

    def pair(src, lo, hi, send, recv, i):
        def sem(sems, k):
            return sems.at[k] if i is None else sems.at[k, i]

        return (
            pltpu.make_async_remote_copy(
                src_ref=src, dst_ref=lo, send_sem=sem(send, 0), recv_sem=sem(recv, 0),
                device_id=(after, m), device_id_type=MESH,
            ),
            pltpu.make_async_remote_copy(
                src_ref=src, dst_ref=hi, send_sem=sem(send, 1), recv_sem=sem(recv, 1),
                device_id=(before, m), device_id_type=MESH,
            ),
        )

    def d_copies(d):
        return pair(od.at[:, cols(d)], lo_h.at[d], hi_h.at[d], d_send, d_recv, d)

    def g_pair(rows, send, recv, i):
        return pair(og.at[rows, :], glo.at[rows, :], ghi.at[rows, :], send, recv, i)

    def rest(i):
        return pl.ds(pl.multiple_of(AWAY + i * REST, 16), REST)

    def g_copies(i):
        return g_pair(rest(i), g_send, g_recv, i)

    def b_copies():
        return g_pair(rows_b, b_send, b_recv, None)

    def u_copies(i):
        rows = cols(i, ROWS)
        return pair(ou.at[rows, :], ulo.at[rows, :], uhi.at[rows, :], u_send, u_recv, i)

    def send(src, dst, send_sem, recv_sem, replica):
        return pltpu.make_async_remote_copy(
            src_ref=src, dst_ref=dst, send_sem=send_sem, recv_sem=recv_sem,
            device_id=(replica, m), device_id_type=MESH,
        )

    def relay_out():
        return send(od.at[early, cols(1)], relayed, relay_sem.at[0], relay_sem.at[1], far_end)

    def relay_over():
        return send(relayed, relayed, relay_sem.at[2], relay_sem.at[1], diagonal)

    def relay_on(first):
        dst, k, where = (lo_h, 0, before) if first else (hi_h, 1, after)
        return send(relayed, dst.at[1, early, :], relay_sem.at[2], d_recv.at[k, 1], where)

    def late_copies():
        return (
            send(od.at[late, cols(1)], lo_h.at[1, late, :], d_send.at[0, 1], d_recv.at[0, 1], after),
            send(od.at[late, cols(1)], hi_h.at[1, late, :], d_send.at[1, 1], d_recv.at[1, 1], before),
        )

    def cross_out(first):
        src, where = (glo, across_down) if first else (ghi, across_up)
        return send(src.at[rows_b, :], crossing, cross_sem.at[0], cross_sem.at[1], where)

    def cross_in(first):
        return send(crossing, summing, cross_sem.at[2], cross_sem.at[3], after if first else before)

    def cross_end(first):
        dst, where = (ghi, before) if first else (glo, after)
        return send(summing, dst.at[rows_b, :], cross_sem.at[4], cross_sem.at[5], where)

    def partial(d, carry):
        part[:, cols(d)] = dot(hid[...], wd[:, cols(d)], ((1,), (0,))).astype(BF16)

        @pl.when(d == 0)
        def _():
            for i in range(n_heads):
                p_copy(*head(i)).start()

        pl.when(d > 0)(p_copy(*block(d)).start)
        return carry

    def join(at, k):
        p_copy(at, k).wait()
        total = part[mine, at].astype(F32) + part_in[:, at].astype(F32)
        part[mine, at] = total.astype(BF16)
        straight = jnp.logical_or(k <= last, inside)
        pl.when(straight)(q_copy(at, k).start)
        pl.when(jnp.logical_not(straight))(detour_out(jnp.maximum(k - last - 1, 0)).start)

    def join_head(i, carry):
        join(*head(i))
        return carry

    def spread(d, carry):
        partial(d, carry)
        join(*block(d - 1))
        return carry

    lax.fori_loop(0, 2, partial, 0)
    lax.fori_loop(0, n_heads, join_head, 0)
    lax.fori_loop(2, n_cols, spread, 0)
    join(*block(n_cols - 1))

    def turn(i, carry):
        hid_t[cols(i), :] = hid[:, cols(i)].T
        return carry

    lax.fori_loop(0, n_units, turn, 0)

    def norm(i, carry):
        rows = cols(i, 64)
        nrm[rows, :] = (x[rows, :].astype(F32) * inv[rows, :]).astype(BF16)
        return carry

    tgt_copy.wait()

    def step_down(at, k):
        q_copy(at, k).wait()

        @pl.when(jnp.logical_and(at_end, k == last))
        def _():
            tell(go_sem, facing)

        total = part[mine, at].astype(F32) + sum_in[:, at].astype(F32)
        offset = x[mine, at].astype(F32) - tg[:, at].astype(F32)
        err[mine, at] = ((offset + total * mid_scale) / toks).astype(BF16)
        e_copy(at, k).start()
        e_copy(at, k).wait()
        grad = dot(hid_t[...], err[:, at], ((1,), (0,)))
        od[:, at] = (wd[:, at].astype(F32) - (step_size * mid_scale) * grad).astype(BF16)

    def inward_start(ahead, behind):
        pl.when(jnp.logical_not(last_end))(ahead.start)
        pl.when(jnp.logical_not(first_end))(behind.start)

    def down_head(i, carry):
        at, k = head(i)
        step_down(at, k)
        inward_start(
            *pair(od.at[:, at], lo_h.at[0, :, at], hi_h.at[0, :, at], d_send, d_recv, 0)
        )
        return carry

    def down(d, carry):
        @pl.when(jnp.logical_and(inside, d <= DETOUR))
        def _():
            i = jnp.minimum(d, DETOUR) - 1
            detour_out(i).wait_recv()
            detour_on(i).start()

        step_down(*block(d))

        @pl.when(d != 1)
        def _():
            inward_start(*d_copies(d))

        @pl.when(d == 1)
        def _():
            ahead, behind = d_copies(1)
            late_ahead, late_behind = late_copies()
            pl.when(along <= 1)(ahead.start)
            pl.when(along >= 2)(behind.start)
            pl.when(along == 2)(late_ahead.start)
            pl.when(along == 1)(late_behind.start)
            pl.when(at_end)(relay_out().start)

        return carry

    def down_late(d, carry):
        step_down(*block(d))
        for copy in d_copies(d):
            copy.start()
        return carry

    lax.fori_loop(0, n_heads, down_head, 0)
    lax.fori_loop(1, n_cols - DETOUR, down, 0)

    @pl.when(at_end)
    def _():
        pl.semaphore_wait(go_sem, len(facing))

    def held_back(d, carry):
        ahead, behind = d_copies(d)
        pl.when(last_end)(ahead.start)
        pl.when(first_end)(behind.start)
        return carry

    held_back(0, 0)
    ahead, behind = late_copies()
    pl.when(last_end)(ahead.start)
    pl.when(first_end)(behind.start)
    lax.fori_loop(2, n_cols - DETOUR, held_back, 0)
    lax.fori_loop(n_cols - DETOUR, n_cols, down_late, 0)

    def back(f, carry):
        grad = dot(err[...], wd[cols(f), :], ((1,), (1,))) * mid_scale
        gg[:, cols(f)] = (grad * slope[:, cols(f)]).astype(BF16)
        gu[:, cols(f)] = (grad * act[:, cols(f)]).astype(BF16)
        return carry

    lax.fori_loop(0, n_units, back, 0)

    @pl.when(at_end)
    def _():
        relay_out().wait_recv()
        relay_over().start()

    lax.fori_loop(0, toks // 64, norm, 0)

    def step(out, grads, rows):
        grad = dot(nrm[:, rows], grads[...], ((0,), (0,)))
        out[rows, :] = (out[rows, :].astype(F32) - (step_size * in_scale) * grad).astype(BF16)

    def step_up(i, carry):
        step(ou, gu, cols(i, ROWS))
        return carry

    def send_up(i, carry):
        for copy in u_copies(i):
            copy.start()
        return carry

    lower, upper = along <= 1, along >= 2
    first_in, last_in = along == 1, along == 2

    def step_gate(i, carry):
        step(og, gg, pl.ds(pl.multiple_of(i * 128, 128), 128))
        return carry

    def send_gate(i, carry):
        for copy in g_copies(i):
            copy.start()
        return carry

    lax.fori_loop(0, width // 128, step_gate, 0)
    ahead, behind = b_copies()
    pl.when(lower)(ahead.start)
    pl.when(upper)(behind.start)
    lax.fori_loop(0, n_rest, send_gate, 0)
    lax.fori_loop(0, n_rows, step_up, 0)

    def third(lo, own, hi):
        return ((lo.astype(F32) + own.astype(F32) + hi.astype(F32)) / 3.0).astype(BF16)

    def mix_down(d, carry):
        for copy in d_copies(d):
            copy.wait()
        loads = [
            pltpu.make_async_copy(lo_h.at[d], stage.at[0], st_sem.at[0]),
            pltpu.make_async_copy(hi_h.at[d], stage.at[1], st_sem.at[1]),
        ]
        for load in loads:
            load.start()
        for load in loads:
            load.wait()
        od[:, cols(d)] = third(stage[0], od[:, cols(d)], stage[1])
        return carry

    mix_down(0, 0)
    lax.fori_loop(2, n_cols, mix_down, 0)

    @pl.when(inside)
    def _():
        relay_out().wait_recv()
        both = relayed[...].astype(F32) + od[early, cols(1)].astype(F32)
        relayed[...] = both.astype(BF16)
        pl.when(first_in)(relay_on(True).start)
        pl.when(last_in)(relay_on(False).start)
        for copy in b_copies():
            copy.wait_recv()
        pl.when(first_in)(cross_out(True).start)
        pl.when(last_in)(cross_out(False).start)
        cross_out(True).wait_recv()
        pl.when(first_in)(cross_in(True).start)
        pl.when(last_in)(cross_in(False).start)

    lax.fori_loop(0, n_rows, send_up, 0)

    def mix(out, lo, hi, rows):
        out[rows, :] = third(lo[rows, :], out[rows, :], hi[rows, :])

    def mix_gate(i, carry):
        for copy in g_copies(i):
            copy.wait()
        mix(og, glo, ghi, rest(i))
        return carry

    lax.fori_loop(0, n_rest, mix_gate, 0)
    ahead, behind = d_copies(1)
    late_ahead, late_behind = late_copies()
    pl.when(lower)(ahead.wait_send)
    pl.when(upper)(behind.wait_send)
    pl.when(upper)(late_ahead.wait_send)
    pl.when(lower)(late_behind.wait_send)
    pl.when(at_end)(relay_out().wait_send)
    pl.when(jnp.logical_not(last_end))(ahead.wait_recv)
    pl.when(jnp.logical_not(first_end))(behind.wait_recv)
    pl.when(last_end)(late_ahead.wait_recv)
    pl.when(first_end)(late_behind.wait_recv)

    def load_second(rows, k):
        held = hi_h if k else lo_h
        return pltpu.make_async_copy(held.at[1, rows, :], stage.at[k, rows, :], st_sem.at[k])

    def third_second(rows):
        loads = [load_second(rows, k) for k in range(2)]
        for load in loads:
            load.start()
        for load in loads:
            load.wait()
        od[rows, cols(1)] = third(stage[0, rows, :], od[rows, cols(1)], stage[1, rows, :])

    third_second(late)

    @pl.when(inside)
    def _():
        third_second(early)

    def end(own, both):
        return ((own.astype(F32) + both.astype(F32)) / 3.0).astype(BF16)

    def end_second(k):
        load = load_second(early, k)
        load.start()
        load.wait()
        od[early, cols(1)] = end(od[early, cols(1)], stage[k, early, :])

    @pl.when(first_end)
    def _():
        end_second(0)

    @pl.when(last_end)
    def _():
        end_second(1)

    ahead, behind = b_copies()
    pl.when(lower)(ahead.wait_send)
    pl.when(upper)(behind.wait_send)

    @pl.when(inside)
    def _():
        cross_in(True).wait_recv()
        both = summing[...].astype(F32) + og[rows_b, :].astype(F32)
        summing[...] = both.astype(BF16)
        pl.when(first_in)(cross_end(True).start)
        pl.when(last_in)(cross_end(False).start)
        cross_out(True).wait_send()
        mix(og, glo, ghi, rows_b)

    def mix_up(i, carry):
        for copy in u_copies(i):
            copy.wait()
        mix(ou, ulo, uhi, cols(i, ROWS))
        return carry

    lax.fori_loop(0, n_rows, mix_up, 0)

    relay_over().wait_send()

    @pl.when(inside)
    def _():
        for i in range(DETOUR):
            detour_on(i).wait_send()

    @pl.when(inside)
    def _():
        cross_in(True).wait_send()
        cross_end(True).wait_send()

    @pl.when(first_end)
    def _():
        cross_end(True).wait_recv()
        og[rows_b, :] = end(og[rows_b, :], ghi[rows_b, :])

    @pl.when(last_end)
    def _():
        cross_end(False).wait_recv()
        og[rows_b, :] = end(og[rows_b, :], glo[rows_b, :])


def write_kernel(pieces, *refs):
    held, out, sem = refs[:3], refs[3:6], refs[6]
    copies = []
    for i in range(3):
        rows = held[i].shape[0] // pieces
        for p in range(pieces):
            part = pl.ds(p * rows, rows)
            copies.append(
                pltpu.make_async_copy(held[i].at[part, :], out[i].at[0, part, :], sem.at[i, p])
            )
    for copy in copies:
        copy.start()
    for copy in copies:
        copy.wait()


def write_out(*arrays):
    pieces = 4
    return pl.pallas_call(
        functools.partial(write_kernel, pieces),
        out_shape=tuple(jax.ShapeDtypeStruct((1, *a.shape), a.dtype) for a in arrays),
        in_specs=[pl.BlockSpec(memory_space=pltpu.VMEM)] * 3,
        out_specs=(pl.BlockSpec(memory_space=pl.ANY),) * 3,
        scratch_shapes=[pltpu.SemaphoreType.DMA((3, pieces))],
        compiler_params=pltpu.CompilerParams(vmem_limit_bytes=16 * 2**20),
    )(*arrays)


def local(replicas, tokens, targets, gate_weight, up_weight, down_weight):
    toks, width = tokens.shape[1:]
    units = gate_weight.shape[2]
    n_cols, n_rows, n_units = width // COLS, width // ROWS, units // COLS
    n_rest = (width - AWAY) // REST
    half = toks // 2
    dma = pltpu.SemaphoreType.DMA
    any_spec = pl.BlockSpec(memory_space=pl.ANY)
    vmem_spec = pl.BlockSpec(memory_space=pltpu.VMEM)
    received = jax.ShapeDtypeStruct((n_cols, units, COLS), BF16)
    gate_out, up_out, down_out, *_ = pl.pallas_call(
        functools.partial(kernel, replicas),
        out_shape=(
            pltpu.VMEM((width, units), BF16),
            pltpu.VMEM((width, units), BF16),
            pltpu.VMEM((units, width), BF16),
            received,
            received,
        ),
        in_specs=[any_spec] * 5,
        out_specs=(vmem_spec, vmem_spec, vmem_spec, any_spec, any_spec),
        scratch_shapes=[
            pltpu.VMEM((toks, width), BF16),
            pltpu.VMEM((half, width), BF16),
            pltpu.VMEM((toks, 1), F32),
            pltpu.VMEM((toks, width), BF16),
            pltpu.VMEM((units, width), BF16),
            pltpu.VMEM((toks, units), F32),
            pltpu.VMEM((toks, units), F32),
            pltpu.VMEM((toks, units), BF16),
            pltpu.VMEM((units, toks), BF16),
            pltpu.VMEM((toks, width), BF16),
            pltpu.VMEM((toks, units), BF16),
            pltpu.VMEM((toks, units), BF16),
            pltpu.VMEM((toks, width), BF16),
            pltpu.VMEM((half, width), BF16),
            pltpu.VMEM((half, width), BF16),
            pltpu.VMEM((DETOUR, half, COLS), BF16),
            pltpu.VMEM((width, units), BF16),
            pltpu.VMEM((width, units), BF16),
            pltpu.VMEM((width, units), BF16),
            pltpu.VMEM((width, units), BF16),
            pltpu.VMEM((2, units, COLS), BF16),
            pltpu.VMEM((AWAY, units), BF16),
            pltpu.VMEM((AWAY, units), BF16),
            pltpu.VMEM((FIRST, COLS), BF16),
            dma((4,)),
            dma((2,)),
            dma((2, n_units)),
            dma((n_cols + COLS // HEAD - 1,)),
            dma((n_cols + COLS // HEAD - 1,)),
            dma((n_cols + COLS // HEAD - 1,)),
            dma((n_cols + COLS // HEAD - 1,)),
            dma((n_cols + COLS // HEAD - 1,)),
            dma((n_cols + COLS // HEAD - 1,)),
            dma((2, n_cols)),
            dma((2, n_cols)),
            dma((2, n_rest)),
            dma((2, n_rest)),
            dma((2, n_rows)),
            dma((2, n_rows)),
            dma((2,)),
            dma((2,)),
            dma((2,)),
            dma((3,)),
            dma((6,)),
            dma((2, DETOUR)),
            pltpu.SemaphoreType.REGULAR,
        ],
        compiler_params=pltpu.CompilerParams(
            collective_id=0, has_side_effects=True, vmem_limit_bytes=50 * 2**20
        ),
    )(tokens[0], targets[0], gate_weight[0], up_weight[0], down_weight[0])
    return write_out(gate_out, up_out, down_out)


def solution(mesh):
    placed = (
        P("gossip", None, None),
        P("gossip", None, None),
        P("gossip", None, "mp"),
        P("gossip", None, "mp"),
        P("gossip", "mp", None),
    )
    return jax.shard_map(
        functools.partial(local, mesh.shape["gossip"]),
        mesh=mesh,
        in_specs=placed,
        out_specs=(P("gossip", None, "mp"), P("gossip", None, "mp"), P("gossip", "mp", None)),
        check_vma=False,
    )
```
